256 devices in a mesh: row: 8 (over y, core), col: 8 (over z), depth: 4 (over x).
Axes of the slice: x: 4, y: 4, z: 8, core: 2. Of those that a mesh axis runs over, the one named last changes fastest.
Arguments:
- matrix: float32 [4, 8, 512, 16384], P(None, 'row', None, ('col', 'depth')), as said below
Outputs:
- factored: float32 [4, 8, 512, 16384], P(None, 'row', None, ('col', 'depth'))
Inputs may be any that keep to these rules, and one draw needn't show every extreme that they name: matrix is symmetric positive definite.
All inputs are finite; a program needn't handle non-finite values.
Results may differ from the reference program's by a relative error of at most 0.0001.
Values sent between devices are 32-bit elements; how exact they have to be, the bound alone decides.
No kernel may reach another device: no remote copies, remote signals or barrier semaphores. Data moves between devices by JAX's collectives and lax.ppermute only.
A program may use at most 128 MiB of HBM per device.

```python
import math
import jax
import jax.numpy as jnp
from jax import lax

B = 512
PANELS = 2
RB = 4
NBLK = 32
ORDER = 16384
N_ROW = 8


def draw_matrix(key, part):
    key_normal = jax.random.fold_in(key, 11)
    key_diagonal = jax.random.fold_in(key, 12)
    latent = 4 * B
    gaussian = jax.random.normal(key_normal, (ORDER, latent), jnp.float32)
    product = jnp.dot(gaussian, gaussian.T, precision=lax.Precision.HIGHEST) / math.sqrt(latent)
    symmetric = (product + product.T) * 0.5
    diag_shift = jax.random.uniform(key_diagonal, (ORDER,), jnp.float32, 0.1, 0.3) * math.sqrt(latent)
    positions = jnp.arange(ORDER)
    symmetric = symmetric.at[positions, positions].add(diag_shift)
    return symmetric.reshape(RB, N_ROW, B, ORDER)


def setup_inputs(seed: int = 0) -> dict:
    seeds = jax.random.split(jax.random.key(seed), 2)
    return {
        "matrix": draw_matrix(jax.random.fold_in(seeds[1], 71), 0),
    }


def factor_blocks(lower_factor, blocks, block_ids, panel_index):
    count_rows, block_size, _ = blocks.shape
    solved = lax.linalg.triangular_solve(lower_factor, blocks.reshape(count_rows * block_size, block_size), left_side=False, lower=True, transpose_a=True)
    solved = solved.reshape(count_rows, block_size, block_size)
    marks = block_ids[:, None, None]
    return jnp.where(marks > panel_index, solved, jnp.where(marks == panel_index, lower_factor[None], jnp.float32(0.0)))

def reference(matrix):
    matrix_full = matrix.reshape(ORDER, ORDER)
    for panel_index in range(PANELS):
        start_col = panel_index * B
        stop_col = start_col + B
        lower_factor = jnp.linalg.cholesky(matrix_full[start_col:stop_col, start_col:stop_col])
        blocks = matrix_full[:, start_col:stop_col].reshape(NBLK, B, B)
        panel_full = factor_blocks(lower_factor, blocks, jnp.arange(NBLK, dtype=jnp.int32), panel_index).reshape(ORDER, B)
        trailing = matrix_full[:, stop_col:] - jnp.dot(panel_full, panel_full[stop_col:].T, precision=lax.Precision.HIGHEST)
        below_rows = (jnp.arange(ORDER, dtype=jnp.int32) >= stop_col)[:, None]
        trailing = jnp.where(below_rows, trailing, jnp.float32(0.0))
        matrix_full = jnp.concatenate([matrix_full[:, :start_col], panel_full, trailing], axis=1)
    return matrix_full.reshape(RB, N_ROW, B, ORDER)
```

```python
import jax
import jax.numpy as jnp
from jax import lax
from jax.experimental import pallas as pl
from jax.experimental.pallas import tpu as pltpu
from jax.sharding import PartitionSpec as P

HI = lax.Precision.HIGHEST
NB = 32
OB = 128
AXES = ("row", "col", "depth")
N_ROW = 8
N_COL = 8
N_DEPTH = 4
N_BC = N_COL * N_DEPTH


def dev(r, c):
    return r * N_BC + c


def at(y, core, z, x):
    return dev(2 * y + core, z * N_DEPTH + x)


OWNER = dev(0, 0)
ROOT = dev(1, 0)


def dot(a, b, ca, cb, precision=HI):
    return lax.dot_general(
        a, b, (((ca,), (cb,)), ((), ())), precision=precision, preferred_element_type=jnp.float32
    )


def eliminate(rows, lane0):
    lanes = lax.broadcasted_iota(jnp.int32, (NB, OB), 1)
    subl = lax.broadcasted_iota(jnp.int32, (NB, OB), 0)
    ident = jnp.where(lanes == subl + lane0, jnp.float32(1.0), jnp.float32(0.0))
    groups = NB // 8

    def split(v):
        return [v[8 * g : 8 * g + 8] for g in range(groups)]

    cols = [
        split(jnp.broadcast_to(rows[:, lane0 + j : lane0 + j + 1], (NB, OB))) for j in range(NB)
    ]
    a = split(rows)
    x = split(ident)
    sub8 = lax.broadcasted_iota(jnp.int32, (8, OB), 0)
    for j in range(NB):
        gj, rj = j // 8, j % 8
        inv = lax.rsqrt(jnp.broadcast_to(cols[j][gj][rj : rj + 1], (8, OB)))
        lcol = [cols[j][g] * inv if g >= gj else None for g in range(groups)]
        ua = jnp.broadcast_to(a[gj][rj : rj + 1], (8, OB)) * inv
        ux = jnp.broadcast_to(x[gj][rj : rj + 1], (8, OB)) * inv
        mine = sub8 == rj
        if rj < 7:
            lself = jnp.where(sub8 > rj, lcol[gj], 0.0)
            a[gj] = jnp.where(mine, ua, a[gj] - lself * ua)
            x[gj] = jnp.where(mine, ux, x[gj] - lself * ux)
        else:
            a[gj] = jnp.where(mine, ua, a[gj])
            x[gj] = jnp.where(mine, ux, x[gj])
        for g in range(gj + 1, groups):
            a[g] = a[g] - lcol[g] * ua
            x[g] = x[g] - lcol[g] * ux
        for k in range(j + 1, NB):
            gk, rk = k // 8, k % 8
            s = jnp.broadcast_to(lcol[gk][rk : rk + 1], (8, OB))
            for g in range(gk, groups):
                cols[k][g] = cols[k][g] - lcol[g] * s
    return jnp.concatenate(a, axis=0), jnp.concatenate(x, axis=0)


def diag_block(w):
    n = OB // NB
    lanes = lax.broadcasted_iota(jnp.int32, (NB, OB), 1)
    subl = lax.broadcasted_iota(jnp.int32, (NB, OB), 0)
    wl = lax.broadcasted_iota(jnp.int32, (OB, OB), 1)
    ups = []
    done = []
    for i in range(n):
        lo = NB * i
        ua, ux = eliminate(w[lo : lo + NB], lo)
        inblk = (lanes >= lo) & (lanes < lo + NB)
        ups.append(jnp.where(lanes >= subl + lo, ua, 0.0))
        u = jnp.where(inblk, jnp.where(lanes <= subl + lo, ux, 0.0), ua)
        if i + 1 < n:
            um = jnp.where(lanes >= lo + NB, u, 0.0)
            w = jnp.where((wl >= lo) & (wl < lo + NB), 0.0, w) - dot(um, u, 0, 0)
        done.append(u)
        w = jnp.concatenate(done + [w[NB * (i + 1) :]] if i + 1 < n else done, axis=0)
    return w, jnp.concatenate(ups, axis=0)


def chol_body(inv_ref, up_ref, m):
    size = m.shape[0]
    nb = size // OB
    up_ref[...] = jnp.zeros((size, size), jnp.float32)
    il = lax.broadcasted_iota(jnp.int32, (OB, OB), 1)
    isb = lax.broadcasted_iota(jnp.int32, (OB, OB), 0)
    lane = lax.broadcasted_iota(jnp.int32, (OB, size), 1)

    def step(b, carry):
        off = pl.multiple_of(b * OB, OB)
        here = pl.ds(off, OB)
        inv, up = diag_block(m[here, here])
        inv = jnp.where(il <= isb, inv, 0.0)
        m[here, here] = jnp.where(il == isb, jnp.float32(1.0), jnp.float32(0.0))
        u = dot(inv, m[here, :], 1, 0)
        m[here, :] = u
        up_ref[here, :] = jnp.where(lane >= off + OB, u, 0.0)
        up_ref[here, here] = up

        def trail(k, c):
            there = pl.ds(pl.multiple_of(k * OB, OB), OB)
            prev = jnp.where((lane >= off) & (lane < off + OB), 0.0, m[there, :])
            m[there, :] = prev - dot(m[here, there], u, 0, 0)
            return c

        lax.fori_loop(b + 1, nb, trail, 0)
        return carry

    lax.fori_loop(0, nb, step, 0)
    row = lax.broadcasted_iota(jnp.int32, (size, size), 0)
    col = lax.broadcasted_iota(jnp.int32, (size, size), 1)
    inv_ref[...] = jnp.where(col <= row, m[...], 0.0)


def lead_kernel(flag, f00, f10, f11, inv, up, m):
    @pl.when(flag[0] == 1)
    def _():
        m[...] = f00[...]
        chol_body(inv.at[0], up.at[0], m)
        q = dot(inv[0], f10[...], 1, 1)
        m[...] = f11[...] - dot(q, q, 0, 0)
        chol_body(inv.at[1], up.at[1], m)


def lead_factors(flag, f00, f10, f11):
    size = f00.shape[0]
    out = jax.ShapeDtypeStruct((2, size, size), jnp.float32)
    vm = pl.BlockSpec(memory_space=pltpu.VMEM)
    return pl.pallas_call(
        lead_kernel,
        out_shape=(out, out),
        in_specs=[pl.BlockSpec(memory_space=pltpu.SMEM), vm, vm, vm],
        out_specs=(vm, vm),
        scratch_shapes=[pltpu.VMEM((size, size), jnp.float32)],
        compiler_params=pltpu.CompilerParams(vmem_limit_bytes=40 << 20),
        name="lead_factors",
    )(flag, f00, f10, f11)


def send(v, pairs):
    return lax.ppermute(v, AXES, pairs)


def broadcast(pieces, me, z):
    piece = jnp.where(me == ROOT, pieces[0], 0.0)
    for k in range(1, N_COL):
        piece = piece + send(pieces[k], [(ROOT, at(0, 1, k, 0))])
    cols = range(N_COL)
    piece = piece + send(piece, [(at(0, 1, k, 0), at(2, 1, k, 0)) for k in cols])
    piece = piece + send(piece, [(at(y, 1, k, 0), at(y + 1, 1, k, 0)) for k in cols for y in (0, 2)])
    piece = piece + send(piece, [(at(y, 1, k, 0), at(y, 1, k, 2)) for k in cols for y in range(4)])
    piece = piece + send(
        piece, [(at(y, 1, k, x), at(y, 1, k, x + 1)) for k in cols for y in range(4) for x in (0, 2)]
    )
    got = [piece]
    for s in range(1, N_COL):
        pairs = [
            (at(y, 1, k, x), at(y, 1, (k + s) % N_COL, x))
            for k in cols
            for y in range(4)
            for x in range(4)
        ]
        got.append(send(piece, pairs))
    order = jnp.stack(got[::-1] + got[::-1])
    full = lax.dynamic_slice_in_dim(order, N_COL - 1 - z, N_COL, 0)
    pairs = [
        (at(y, 1, k, x), at(y, 0, k, x)) for k in cols for y in range(4) for x in range(4)
    ]
    pairs = [p for p in pairs if p[1] != OWNER]
    other = send(full, pairs)
    return jnp.where((me // N_BC) % 2 == 1, full, other)


def body(matrix):
    blocks = matrix[:, 0, :, :]
    count, size, _ = blocks.shape
    r = lax.axis_index("row")
    z = lax.axis_index("col")
    c = lax.axis_index(("col", "depth"))
    me = lax.axis_index(AXES)
    owner = me == OWNER
    mine = blocks[0]

    f10 = send(mine, [(ROOT, OWNER)])
    f11 = send(mine, [(dev(1, 1), OWNER)])

    step = size // 8
    got = []
    for k in range(8):
        pairs = [(dev(0, j), dev(j % 8, 8 * (j // 8) + k)) for j in range(1, N_BC)]
        pairs += [(dev(1, j), dev(j % 8, 8 * (j // 8) + (k + 4) % 8)) for j in range(1, N_BC)]
        part = mine
        sent = jnp.where(
            r == 0,
            part[k * step : (k + 1) * step],
            part[((k + 4) % 8) * step : ((k + 4) % 8 + 1) * step],
        )
        got.append(send(sent, pairs))
    slot = c % 8
    first = sum(jnp.where(slot == k, got[k], 0.0) for k in range(8))
    second = sum(jnp.where(slot == (k + 4) % 8, got[k], 0.0) for k in range(8))
    gathered = lax.all_gather(jnp.stack([first, second]), ("col", "depth"))
    gathered = gathered.reshape(count, 2 * size, size)

    cs = range(2, N_BC)
    line = mine
    line = jnp.where(r < 2, line, 0.0)
    line = line + send(mine, [(dev(a, j), dev(a + 2, j)) for j in cs for a in (0, 1)])
    line = line + send(mine, [(dev(a, j), dev(a + 6, j)) for j in cs for a in (0, 1)])
    line = line + send(line, [(dev(a + 2, j), dev(a + 4, j)) for j in cs for a in (0, 1)])
    swap = send(line, [(dev(a, j), dev(a ^ 1, j)) for j in cs for a in range(8)])
    even = r % 2 == 0
    w0 = jnp.where(even, line, swap)
    w1 = jnp.where(even, swap, line)

    flag = owner.astype(jnp.int32).reshape(1)
    inv, up = lead_factors(flag, mine, f10, f11)
    l1_up = send(up[1], [(OWNER, dev(1, 1))])
    inv_root = send(inv, [(OWNER, ROOT)])
    cross = broadcast(mine.reshape(8, step, size), me, z).reshape(size, size)
    cross = jnp.where(owner, f10, cross)
    inv_all = broadcast(inv_root.reshape(8, 2 * step, size), me, z).reshape(2, size, size)
    inv_all = jnp.where(owner, inv, inv_all)
    i0, i1 = inv_all[0], inv_all[1]

    eye = jnp.eye(size, dtype=jnp.float32)
    q0 = dot(i0, w0, 1, 0)
    q0 = jnp.where(c == 0, -eye, jnp.where(c == 1, 0.0, q0))
    x0 = dot(i0, q0, 0, 0)
    link = dot(i0, dot(i0, cross, 1, 1), 0, 0)
    q1 = dot(i1, w1 - dot(cross, x0, 1, 0), 1, 0)
    q1 = jnp.where(c == 0, 0.0, jnp.where(c == 1, -eye, q1))
    y1 = -dot(i1, q1, 0, 0)
    y0 = -x0 - dot(link, y1, 1, 0)
    y = jnp.stack([y0.reshape(8, step, size), y1.reshape(8, step, size)], axis=1).reshape(2 * size, size)

    ids = jnp.arange(count, dtype=jnp.int32) * N_ROW + r
    keep = (ids > jnp.minimum(c, 1))[:, None, None]
    product = jnp.einsum("akx,ky->axy", gathered, y, precision=lax.Precision.HIGH)
    out = jnp.where(keep, jnp.where(c >= 2, blocks, 0.0) + product, 0.0)
    diag = jnp.where(owner, up[0], l1_up).T
    head = jnp.where(owner | (me == dev(1, 1)), diag, out[0])
    out = jnp.concatenate([head[None], out[1:]], axis=0)
    return out[:, None, :, :]


def solution(mesh):
    placed = P(None, "row", None, ("col", "depth"))
    return jax.shard_map(body, mesh=mesh, in_specs=(placed,), out_specs=placed, check_vma=False)
```

```python
import jax
import jax.numpy as jnp
from jax import lax
from jax.experimental import pallas as pl
from jax.experimental.pallas import tpu as pltpu
from jax.sharding import PartitionSpec as P

HI = lax.Precision.HIGHEST
NB = 32
OB = 128
AXES = ("row", "col", "depth")
N_ROW = 8
N_COL = 8
N_DEPTH = 4
N_BC = N_COL * N_DEPTH


def dev(r, c):
    return r * N_BC + c


def at(y, core, z, x):
    return dev(2 * y + core, z * N_DEPTH + x)


OWNER = dev(0, 0)
ROOT = dev(1, 0)


def dot(a, b, ca, cb, precision=HI):
    return lax.dot_general(
        a, b, (((ca,), (cb,)), ((), ())), precision=precision, preferred_element_type=jnp.float32
    )


def eliminate(rows, lane0):
    lanes = lax.broadcasted_iota(jnp.int32, (NB, OB), 1)
    subl = lax.broadcasted_iota(jnp.int32, (NB, OB), 0)
    ident = jnp.where(lanes == subl + lane0, jnp.float32(1.0), jnp.float32(0.0))
    groups = NB // 8

    def split(v):
        return [v[8 * g : 8 * g + 8] for g in range(groups)]

    cols = [
        split(jnp.broadcast_to(rows[:, lane0 + j : lane0 + j + 1], (NB, OB))) for j in range(NB)
    ]
    a = split(rows)
    x = split(ident)
    sub8 = lax.broadcasted_iota(jnp.int32, (8, OB), 0)
    for j in range(NB):
        gj, rj = j // 8, j % 8
        inv = lax.rsqrt(jnp.broadcast_to(cols[j][gj][rj : rj + 1], (8, OB)))
        lcol = [cols[j][g] * inv if g >= gj else None for g in range(groups)]
        ua = jnp.broadcast_to(a[gj][rj : rj + 1], (8, OB)) * inv
        ux = jnp.broadcast_to(x[gj][rj : rj + 1], (8, OB)) * inv
        mine = sub8 == rj
        if rj < 7:
            lself = jnp.where(sub8 > rj, lcol[gj], 0.0)
            a[gj] = jnp.where(mine, ua, a[gj] - lself * ua)
            x[gj] = jnp.where(mine, ux, x[gj] - lself * ux)
        else:
            a[gj] = jnp.where(mine, ua, a[gj])
            x[gj] = jnp.where(mine, ux, x[gj])
        for g in range(gj + 1, groups):
            a[g] = a[g] - lcol[g] * ua
            x[g] = x[g] - lcol[g] * ux
        for k in range(j + 1, NB):
            gk, rk = k // 8, k % 8
            s = jnp.broadcast_to(lcol[gk][rk : rk + 1], (8, OB))
            for g in range(gk, groups):
                cols[k][g] = cols[k][g] - lcol[g] * s
    return jnp.concatenate(a, axis=0), jnp.concatenate(x, axis=0)


def diag_block(w):
    n = OB // NB
    lanes = lax.broadcasted_iota(jnp.int32, (NB, OB), 1)
    subl = lax.broadcasted_iota(jnp.int32, (NB, OB), 0)
    wl = lax.broadcasted_iota(jnp.int32, (OB, OB), 1)
    ups = []
    done = []
    for i in range(n):
        lo = NB * i
        ua, ux = eliminate(w[lo : lo + NB], lo)
        inblk = (lanes >= lo) & (lanes < lo + NB)
        ups.append(jnp.where(lanes >= subl + lo, ua, 0.0))
        u = jnp.where(inblk, jnp.where(lanes <= subl + lo, ux, 0.0), ua)
        if i + 1 < n:
            um = jnp.where(lanes >= lo + NB, u, 0.0)
            w = jnp.where((wl >= lo) & (wl < lo + NB), 0.0, w) - dot(um, u, 0, 0)
        done.append(u)
        w = jnp.concatenate(done + [w[NB * (i + 1) :]] if i + 1 < n else done, axis=0)
    return w, jnp.concatenate(ups, axis=0)


def chol_body(inv_ref, up_ref, m):
    size = m.shape[0]
    nb = size // OB
    up_ref[...] = jnp.zeros((size, size), jnp.float32)
    il = lax.broadcasted_iota(jnp.int32, (OB, OB), 1)
    isb = lax.broadcasted_iota(jnp.int32, (OB, OB), 0)
    lane = lax.broadcasted_iota(jnp.int32, (OB, size), 1)

    def step(b, carry):
        off = pl.multiple_of(b * OB, OB)
        here = pl.ds(off, OB)
        inv, up = diag_block(m[here, here])
        inv = jnp.where(il <= isb, inv, 0.0)
        m[here, here] = jnp.where(il == isb, jnp.float32(1.0), jnp.float32(0.0))
        u = dot(inv, m[here, :], 1, 0)
        m[here, :] = u
        up_ref[here, :] = jnp.where(lane >= off + OB, u, 0.0)
        up_ref[here, here] = up

        def trail(k, c):
            there = pl.ds(pl.multiple_of(k * OB, OB), OB)
            prev = jnp.where((lane >= off) & (lane < off + OB), 0.0, m[there, :])
            m[there, :] = prev - dot(m[here, there], u, 0, 0)
            return c

        lax.fori_loop(b + 1, nb, trail, 0)
        return carry

    lax.fori_loop(0, nb, step, 0)
    row = lax.broadcasted_iota(jnp.int32, (size, size), 0)
    col = lax.broadcasted_iota(jnp.int32, (size, size), 1)
    inv_ref[...] = jnp.where(col <= row, m[...], 0.0)


def pack(inv, packed):
    size = inv.shape[0]
    for p in range(8):
        wide = OB * (p // 4 + 1)
        packed[p, :, :wide] = inv[NB * p : NB * (p + 1), :wide]
        packed[p, :, wide:] = inv[size - NB * (p + 1) : size - NB * p, : size + OB - wide]


def unpack(packed, inv, z):
    size = inv.shape[0]
    inv[...] = jnp.zeros((size, size), jnp.float32)
    for p in range(8):
        wide = OB * (p // 4 + 1)
        piece = packed[lax.bitwise_xor(z, p)]
        inv[NB * p : NB * (p + 1), :wide] = piece[:, :wide]
        inv[size - NB * (p + 1) : size - NB * p, : size + OB - wide] = piece[:, wide:]


def choose(own, mine, got, dst):
    @pl.when(own)
    def _():
        dst(mine)

    @pl.when(jnp.logical_not(own))
    def _():
        dst(got)


def middle_kernel(place, line, swap, own0, got0, own_cross, got_cross, x0, link, rest, inv, w1):
    c = place[0]
    even = lax.rem(place[1], 2) == 0
    own = place[2] == 1
    size = inv.shape[0]
    choose(own, own0, got0, lambda packed: unpack(packed, inv, place[3]))

    @pl.when(own)
    def _():
        rest[...] = own_cross[...]

    @pl.when(jnp.logical_not(own))
    def _():
        for p in range(8):
            part = size // 8
            rest[part * p : part * (p + 1)] = got_cross[lax.bitwise_xor(place[3], p)]

    def keep(a, b):
        x0[...] = a[...]
        w1[...] = b[...]

    @pl.when(even)
    def _():
        keep(line, swap)

    @pl.when(jnp.logical_not(even))
    def _():
        keep(swap, line)

    il = lax.broadcasted_iota(jnp.int32, (size, size), 1)
    isb = lax.broadcasted_iota(jnp.int32, (size, size), 0)
    eye = jnp.where(il == isb, jnp.float32(1.0), jnp.float32(0.0))
    q0 = dot(inv[...], x0[...], 1, 0)
    q0 = jnp.where(c == 0, -eye, jnp.where(c == 1, 0.0, q0))
    x0[...] = dot(inv[...], q0, 0, 0)
    link[...] = dot(inv[...], dot(inv[...], rest[...], 1, 1), 0, 0)
    rest[...] = w1[...] - dot(rest[...], x0[...], 1, 0)


def tail_kernel(place, own1, got1, x0, link, rest, y, inv):
    c = place[0]
    own = place[2] == 1
    size = inv.shape[0]
    choose(own, own1, got1, lambda packed: unpack(packed, inv, place[3]))
    il = lax.broadcasted_iota(jnp.int32, (size, size), 1)
    isb = lax.broadcasted_iota(jnp.int32, (size, size), 0)
    eye = jnp.where(il == isb, jnp.float32(1.0), jnp.float32(0.0))
    q1 = dot(inv[...], rest[...], 1, 0)
    q1 = jnp.where(c == 0, 0.0, jnp.where(c == 1, -eye, q1))
    y1 = -dot(inv[...], q1, 0, 0)
    y[1] = y1
    y[0] = -x0[...] - dot(link[...], y1, 1, 0)


def multipliers(kernel, outs, scratch, place, *ins):
    vm = pl.BlockSpec(memory_space=pltpu.VMEM)
    return pl.pallas_call(
        kernel,
        out_shape=tuple(jax.ShapeDtypeStruct(o, jnp.float32) for o in outs),
        in_specs=[pl.BlockSpec(memory_space=pltpu.SMEM)] + [vm] * len(ins),
        out_specs=(vm,) * len(outs),
        scratch_shapes=[pltpu.VMEM(o, jnp.float32) for o in scratch],
        compiler_params=pltpu.CompilerParams(vmem_limit_bytes=50 << 20),
        name=kernel.__name__,
    )(place, *ins)


def first_kernel(flag, f00, inv, packed, up, m):
    @pl.when(flag[0] == 1)
    def _():
        m[...] = f00[...]
        chol_body(inv, up, m)
        pack(inv, packed)


def second_kernel(flag, inv0, f10, f11, inv, packed, up, m):
    @pl.when(flag[0] == 1)
    def _():
        q = dot(inv0[...], f10[...], 1, 1)
        m[...] = f11[...] - dot(q, q, 0, 0)
        chol_body(inv, up, m)
        pack(inv, packed)


def factor(kernel, flag, *ins):
    size = ins[0].shape[0]
    out = jax.ShapeDtypeStruct((size, size), jnp.float32)
    packed = jax.ShapeDtypeStruct((8, NB, size + OB), jnp.float32)
    vm = pl.BlockSpec(memory_space=pltpu.VMEM)
    return pl.pallas_call(
        kernel,
        out_shape=(out, packed, out),
        in_specs=[pl.BlockSpec(memory_space=pltpu.SMEM)] + [vm] * len(ins),
        out_specs=(vm, vm, vm),
        scratch_shapes=[pltpu.VMEM((size, size), jnp.float32)],
        compiler_params=pltpu.CompilerParams(vmem_limit_bytes=32 << 20),
        name=kernel.__name__,
    )(flag, *ins)


def halves(v):
    high = v.astype(jnp.bfloat16)
    return high, (v - high.astype(jnp.float32)).astype(jnp.bfloat16)


def last_kernel(place, g, y, f, own_diag, out, yh, yl):
    a = pl.program_id(0)
    h = pl.program_id(1)
    c = place[0]
    ident = a * N_ROW + place[1]
    size = y.shape[1]
    half = size // 2

    @pl.when((a == 0) & (h == 0))
    def _():
        for k, ref in enumerate(halves(y[0])):
            (yh, yl)[k][0] = ref
        for k in range(2):
            for n, ref in enumerate(halves(y[1, half * k : half * (k + 1)])):
                (yh, yl)[n][1, half * (1 - k) : half * (2 - k)] = ref

    rows = out.shape[2]

    def bf(p, q):
        return jnp.dot(p, q, preferred_element_type=jnp.float32)

    row = lax.broadcasted_iota(jnp.int32, (rows, size), 0) + h * rows
    col = lax.broadcasted_iota(jnp.int32, (rows, size), 1)

    @pl.when((ident > jnp.minimum(c, 1)) | ((ident == 1) & (c == 1)))
    def _():
        total = jnp.where(c >= 2, f[0, 0], 0.0)
        for k in range(2):
            high, low = halves(g[:, k].reshape(size, rows).T)
            total = total + (bf(low, yh[k]) + bf(high, yl[k]) + bf(high, yh[k]))
        out[0, 0] = jnp.where((ident == 1) & (c == 1) & (col > row), 0.0, total)

    @pl.when((ident <= jnp.minimum(c, 1)) & ((ident != c) | (c > 1)))
    def _():
        out[0, 0] = jnp.zeros((rows, size), jnp.float32)

    @pl.when((ident == 0) & (c == 0))
    def _():
        out[0, 0] = own_diag[:, pl.ds(pl.multiple_of(h * rows, rows), rows)].T


def last(place, gathered, y, matrix, own_diag):
    count, _, size, _ = matrix.shape
    part = 2
    rows = size // part
    tile = pl.BlockSpec((1, 1, rows, size), lambda a, h: (a, 0, h, 0))
    return pl.pallas_call(
        last_kernel,
        grid=(count, part),
        out_shape=jax.ShapeDtypeStruct(matrix.shape, jnp.float32),
        in_specs=[
            pl.BlockSpec(memory_space=pltpu.SMEM),
            pl.BlockSpec((8, 2, size // 8, rows), lambda a, h: (a, 0, 0, h)),
            pl.BlockSpec((2, size, size), lambda a, h: (0, 0, 0)),
            tile,
            pl.BlockSpec((size, size), lambda a, h: (0, 0)),
        ],
        out_specs=tile,
        scratch_shapes=[pltpu.VMEM((2, size, size), jnp.bfloat16)] * 2,
        compiler_params=pltpu.CompilerParams(vmem_limit_bytes=50 << 20),
        name="last",
    )(place, gathered, y, matrix, own_diag)


def send(v, pairs):
    return lax.ppermute(v, AXES, pairs)


def later(v, first):
    return v + jnp.minimum(jnp.abs(first[(0,) * first.ndim]), 0.0)


def broadcast(pieces, me, ahead=None, start=None):
    cols, ys, xs = range(N_COL), range(4), range(4)
    steps = []

    def wait(v):
        return v if ahead is None else later(v, ahead[len(steps)])

    held = jnp.where(me == ROOT, pieces, 0.0)
    if start is not None:
        held = later(held, start)
    for half in (4, 2, 1):
        pairs = [(at(0, 1, k, 0), at(0, 1, k + half, 0)) for k in range(0, N_COL, 2 * half)]
        held = wait(held)
        held = held[:half] + send(held[half:], pairs)
        steps.append(held)
    for pairs in (
        [(at(0, 1, k, 0), at(2, 1, k, 0)) for k in cols],
        [(at(y, 1, k, 0), at(y + 1, 1, k, 0)) for k in cols for y in (0, 2)],
        [(at(y, 1, k, 0), at(y, 1, k, 2)) for k in cols for y in ys],
        [(at(y, 1, k, x), at(y, 1, k, x + 1)) for k in cols for y in ys for x in (0, 2)],
    ):
        held = wait(held)
        held = held + send(held, pairs)
        steps.append(held)
    for bit in (1, 2, 4):
        pairs = [(at(y, 1, k, x), at(y, 1, k ^ bit, x)) for k in cols for y in ys for x in xs]
        held = wait(held)
        held = jnp.concatenate([held, send(held, pairs)])
        steps.append(held)
    pairs = [(at(y, 1, k, x), at(y, 0, k, x)) for k in cols for y in ys for x in xs]
    held = wait(held)
    other = send(held, [p for p in pairs if p[1] != OWNER])
    steps.append(other)
    return jnp.where((me // N_BC) % 2 == 1, held, other), steps


def body(matrix):
    mine = matrix[0, 0]
    size = mine.shape[0]
    r = lax.axis_index("row")
    z = lax.axis_index("col")
    c = lax.axis_index(("col", "depth"))
    me = lax.axis_index(AXES)
    owner = me == OWNER
    place = jnp.stack([c, r, owner.astype(jnp.int32), z]).astype(jnp.int32)

    step = size // 8
    got = []
    for k in range(8):
        pairs = [(dev(0, j), dev(j % 8, 8 * (j // 8) + k)) for j in range(1, N_BC)]
        pairs += [(dev(1, j), dev(j % 8, 8 * (j // 8) + (k + 4) % 8)) for j in range(1, N_BC)]
        got.append(send(mine[k * step : (k + 1) * step], pairs))
    slot = c % 8
    first = sum(jnp.where(slot == k, got[k], 0.0) for k in range(8))
    second = sum(jnp.where(slot == (k + 4) % 8, got[k], 0.0) for k in range(8))
    f10 = send(mine, [(ROOT, OWNER)])
    f11 = send(mine, [(dev(1, 1), OWNER)])
    shares, mine, f10, f11 = lax.optimization_barrier((jnp.stack([first, second]), mine, f10, f11))
    gathered = lax.all_gather(shares, ("col", "depth"))

    flag = owner.astype(jnp.int32).reshape(1)
    inv0, packed0, up0 = factor(first_kernel, flag, mine)
    root0 = send(packed0, [(OWNER, ROOT)])
    _, packed1, _ = factor(second_kernel, flag, inv0, f10, f11)
    root1 = send(packed1, [(OWNER, ROOT)])
    cross, steps = broadcast(mine.reshape(8, step, size), me)
    got0, steps = broadcast(root0, me, steps)
    spread = steps[6]
    got1, _ = broadcast(root1, me, steps, spread)

    cs = range(2, N_BC)
    line = jnp.where(r < 2, mine, 0.0)
    line = line + send(mine, [(dev(a, j), dev(a + 2, j)) for j in cs for a in (0, 1)])
    line = line + send(mine, [(dev(a, j), dev(a + 6, j)) for j in cs for a in (0, 1)])
    line = later(line, spread)
    line = line + send(line, [(dev(a + 2, j), dev(a + 4, j)) for j in cs for a in (0, 1)])
    swap = send(line, [(dev(a, j), dev(a ^ 1, j)) for j in cs for a in range(8)])

    block = (size, size)
    x0, link, rest = multipliers(
        middle_kernel, [block] * 3, [block] * 2, place, line, swap, packed0, got0, f10, cross
    )
    (y,) = multipliers(tail_kernel, [(2,) + block], [block], place, packed1, got1, x0, link, rest)
    return last(place, gathered, y, matrix, up0)


def solution(mesh):
    placed = P(None, "row", None, ("col", "depth"))
    return jax.shard_map(body, mesh=mesh, in_specs=(placed,), out_specs=placed, check_vma=False)
```

```python
import jax
import jax.numpy as jnp
from jax import lax
from jax.experimental import pallas as pl
from jax.experimental.pallas import tpu as pltpu
from jax.sharding import PartitionSpec as P

HI = lax.Precision.HIGHEST
NB = 32
OB = 128
AXES = ("row", "col", "depth")
N_ROW = 8
N_COL = 8
N_DEPTH = 4
N_BC = N_COL * N_DEPTH


def dev(r, c):
    return r * N_BC + c


def at(y, core, z, x):
    return dev(2 * y + core, z * N_DEPTH + x)


OWNER = dev(0, 0)
ROOT = dev(1, 0)


def dot(a, b, ca, cb, precision=HI):
    return lax.dot_general(
        a, b, (((ca,), (cb,)), ((), ())), precision=precision, preferred_element_type=jnp.float32
    )


def eliminate(rows, lane0):
    lanes = lax.broadcasted_iota(jnp.int32, (NB, OB), 1)
    subl = lax.broadcasted_iota(jnp.int32, (NB, OB), 0)
    ident = jnp.where(lanes == subl + lane0, jnp.float32(1.0), jnp.float32(0.0))
    groups = NB // 8

    def split(v):
        return [v[8 * g : 8 * g + 8] for g in range(groups)]

    cols = [
        split(jnp.broadcast_to(rows[:, lane0 + j : lane0 + j + 1], (NB, OB))) for j in range(NB)
    ]
    a = split(rows)
    x = split(ident)
    sub8 = lax.broadcasted_iota(jnp.int32, (8, OB), 0)
    for j in range(NB):
        gj, rj = j // 8, j % 8
        inv = lax.rsqrt(jnp.broadcast_to(cols[j][gj][rj : rj + 1], (8, OB)))
        lcol = [cols[j][g] * inv if g >= gj else None for g in range(groups)]
        ua = jnp.broadcast_to(a[gj][rj : rj + 1], (8, OB)) * inv
        ux = jnp.broadcast_to(x[gj][rj : rj + 1], (8, OB)) * inv
        mine = sub8 == rj
        if rj < 7:
            lself = jnp.where(sub8 > rj, lcol[gj], 0.0)
            a[gj] = jnp.where(mine, ua, a[gj] - lself * ua)
            x[gj] = jnp.where(mine, ux, x[gj] - lself * ux)
        else:
            a[gj] = jnp.where(mine, ua, a[gj])
            x[gj] = jnp.where(mine, ux, x[gj])
        for g in range(gj + 1, groups):
            a[g] = a[g] - lcol[g] * ua
            x[g] = x[g] - lcol[g] * ux
        for k in range(j + 1, NB):
            gk, rk = k // 8, k % 8
            s = jnp.broadcast_to(lcol[gk][rk : rk + 1], (8, OB))
            for g in range(gk, groups):
                cols[k][g] = cols[k][g] - lcol[g] * s
    return jnp.concatenate(a, axis=0), jnp.concatenate(x, axis=0)


def diag_block(w):
    n = OB // NB
    lanes = lax.broadcasted_iota(jnp.int32, (NB, OB), 1)
    subl = lax.broadcasted_iota(jnp.int32, (NB, OB), 0)
    wl = lax.broadcasted_iota(jnp.int32, (OB, OB), 1)
    ups = []
    done = []
    for i in range(n):
        lo = NB * i
        ua, ux = eliminate(w[lo : lo + NB], lo)
        inblk = (lanes >= lo) & (lanes < lo + NB)
        ups.append(jnp.where(lanes >= subl + lo, ua, 0.0))
        u = jnp.where(inblk, jnp.where(lanes <= subl + lo, ux, 0.0), ua)
        if i + 1 < n:
            um = jnp.where(lanes >= lo + NB, u, 0.0)
            w = jnp.where((wl >= lo) & (wl < lo + NB), 0.0, w) - dot(um, u, 0, 0)
        done.append(u)
        w = jnp.concatenate(done + [w[NB * (i + 1) :]] if i + 1 < n else done, axis=0)
    return w, jnp.concatenate(ups, axis=0)


def chol_body(inv_ref, up_ref, m):
    size = m.shape[0]
    nb = size // OB
    up_ref[...] = jnp.zeros((size, size), jnp.float32)
    il = lax.broadcasted_iota(jnp.int32, (OB, OB), 1)
    isb = lax.broadcasted_iota(jnp.int32, (OB, OB), 0)
    lane = lax.broadcasted_iota(jnp.int32, (OB, size), 1)

    def step(b, carry):
        off = pl.multiple_of(b * OB, OB)
        here = pl.ds(off, OB)
        inv, up = diag_block(m[here, here])
        inv = jnp.where(il <= isb, inv, 0.0)
        m[here, here] = jnp.where(il == isb, jnp.float32(1.0), jnp.float32(0.0))
        u = dot(inv, m[here, :], 1, 0)
        m[here, :] = u
        up_ref[here, :] = jnp.where(lane >= off + OB, u, 0.0)
        up_ref[here, here] = up

        def trail(k, c):
            there = pl.ds(pl.multiple_of(k * OB, OB), OB)
            prev = jnp.where((lane >= off) & (lane < off + OB), 0.0, m[there, :])
            m[there, :] = prev - dot(m[here, there], u, 0, 0)
            return c

        lax.fori_loop(b + 1, nb, trail, 0)
        return carry

    lax.fori_loop(0, nb, step, 0)
    row = lax.broadcasted_iota(jnp.int32, (size, size), 0)
    col = lax.broadcasted_iota(jnp.int32, (size, size), 1)
    inv_ref[...] = jnp.where(col <= row, m[...], 0.0)


def pack(inv, packed):
    size = inv.shape[0]
    for p in range(8):
        wide = OB * (p // 4 + 1)
        packed[p, :, :wide] = inv[NB * p : NB * (p + 1), :wide]
        packed[p, :, wide:] = inv[size - NB * (p + 1) : size - NB * p, : size + OB - wide]


def slot_of(place, p):
    v = lax.bitwise_xor(place[3], p)
    low, high = lax.bitwise_and(v, 1), lax.shift_right_logical(v, 2)
    return jnp.where(place[2] == 1, p, 4 * low + lax.bitwise_and(v, 2) + high)


def unpack(packed, inv, place):
    size = inv.shape[0]
    inv[...] = jnp.zeros((size, size), jnp.float32)
    for p in range(8):
        wide = OB * (p // 4 + 1)
        piece = packed[slot_of(place, p)]
        inv[NB * p : NB * (p + 1), :wide] = piece[:, :wide]
        inv[size - NB * (p + 1) : size - NB * p, : size + OB - wide] = piece[:, wide:]


def choose(place, own, on_one, on_zero, take):
    owner = place[2] == 1
    one = lax.rem(place[1], 2) == 1

    @pl.when(owner)
    def _():
        take(own)

    @pl.when(one)
    def _():
        take(on_one)

    @pl.when(jnp.logical_not(owner | one))
    def _():
        take(on_zero)


def middle_kernel(
    place, line, swap, own0, one0, zero0, own_cross, one_cross, zero_cross, x0, link, rest, inv, w1
):
    c = place[0]
    even = lax.rem(place[1], 2) == 0
    size = inv.shape[0]
    choose(place, own0, one0, zero0, lambda packed: unpack(packed, inv, place))

    def keep_cross(ref):
        part = size // 8
        for p in range(8):
            rest[part * p : part * (p + 1)] = ref[slot_of(place, p)]

    choose(place, own_cross, one_cross, zero_cross, keep_cross)

    def keep(a, b):
        x0[...] = a[...]
        w1[...] = b[...]

    @pl.when(even)
    def _():
        keep(line, swap)

    @pl.when(jnp.logical_not(even))
    def _():
        keep(swap, line)

    il = lax.broadcasted_iota(jnp.int32, (size, size), 1)
    isb = lax.broadcasted_iota(jnp.int32, (size, size), 0)
    eye = jnp.where(il == isb, jnp.float32(1.0), jnp.float32(0.0))
    q0 = dot(inv[...], x0[...], 1, 0)
    q0 = jnp.where(c == 0, -eye, jnp.where(c == 1, 0.0, q0))
    x0[...] = dot(inv[...], q0, 0, 0)
    link[...] = dot(inv[...], dot(inv[...], rest[...], 1, 1), 0, 0)
    rest[...] = w1[...] - dot(rest[...], x0[...], 1, 0)


def tail_kernel(place, own1, one1, zero1, x0, link, rest, y, inv):
    c = place[0]
    size = inv.shape[0]
    choose(place, own1, one1, zero1, lambda packed: unpack(packed, inv, place))
    il = lax.broadcasted_iota(jnp.int32, (size, size), 1)
    isb = lax.broadcasted_iota(jnp.int32, (size, size), 0)
    eye = jnp.where(il == isb, jnp.float32(1.0), jnp.float32(0.0))
    q1 = dot(inv[...], rest[...], 1, 0)
    q1 = jnp.where(c == 0, 0.0, jnp.where(c == 1, -eye, q1))
    y1 = -dot(inv[...], q1, 0, 0)
    y[1] = y1
    y[0] = -x0[...] - dot(link[...], y1, 1, 0)


def multipliers(kernel, outs, scratch, place, *ins):
    vm = pl.BlockSpec(memory_space=pltpu.VMEM)
    return pl.pallas_call(
        kernel,
        out_shape=tuple(jax.ShapeDtypeStruct(o, jnp.float32) for o in outs),
        in_specs=[pl.BlockSpec(memory_space=pltpu.SMEM)] + [vm] * len(ins),
        out_specs=(vm,) * len(outs),
        scratch_shapes=[pltpu.VMEM(o, jnp.float32) for o in scratch],
        compiler_params=pltpu.CompilerParams(vmem_limit_bytes=50 << 20),
        name=kernel.__name__,
    )(place, *ins)


def first_kernel(flag, f00, inv, packed, up, tick, m):
    tick[...] = jnp.zeros(tick.shape, jnp.float32)

    @pl.when(flag[0] == 1)
    def _():
        m[...] = f00[...]
        chol_body(inv, up, m)
        pack(inv, packed)


def second_kernel(flag, inv0, f10, f11, inv, packed, up, tick, m):
    tick[...] = jnp.zeros(tick.shape, jnp.float32)

    @pl.when(flag[0] == 1)
    def _():
        q = dot(inv0[...], f10[...], 1, 1)
        m[...] = f11[...] - dot(q, q, 0, 0)
        chol_body(inv, up, m)
        pack(inv, packed)


def factor(kernel, flag, *ins):
    size = ins[0].shape[0]
    out = jax.ShapeDtypeStruct((size, size), jnp.float32)
    packed = jax.ShapeDtypeStruct((8, NB, size + OB), jnp.float32)
    vm = pl.BlockSpec(memory_space=pltpu.VMEM)
    return pl.pallas_call(
        kernel,
        out_shape=(out, packed, out, jax.ShapeDtypeStruct((8, OB), jnp.float32)),
        in_specs=[pl.BlockSpec(memory_space=pltpu.SMEM)] + [vm] * len(ins),
        out_specs=(vm, vm, vm, vm),
        scratch_shapes=[pltpu.VMEM((size, size), jnp.float32)],
        compiler_params=pltpu.CompilerParams(vmem_limit_bytes=32 << 20),
        name=kernel.__name__,
    )(flag, *ins)


def halves(v):
    high = v.astype(jnp.bfloat16)
    return high, (v - high.astype(jnp.float32)).astype(jnp.bfloat16)


def last_kernel(place, g, y, f, own_diag, out, yh, yl):
    a = pl.program_id(0)
    h = pl.program_id(1)
    c = place[0]
    ident = a * N_ROW + place[1]
    size = y.shape[1]
    half = size // 2

    @pl.when((a == 0) & (h == 0))
    def _():
        for k, ref in enumerate(halves(y[0])):
            (yh, yl)[k][0] = ref
        for k in range(2):
            for n, ref in enumerate(halves(y[1, half * k : half * (k + 1)])):
                (yh, yl)[n][1, half * (1 - k) : half * (2 - k)] = ref

    rows = out.shape[2]

    def bf(p, q):
        return jnp.dot(p, q, preferred_element_type=jnp.float32)

    row = lax.broadcasted_iota(jnp.int32, (rows, size), 0) + h * rows
    col = lax.broadcasted_iota(jnp.int32, (rows, size), 1)

    @pl.when((ident > jnp.minimum(c, 1)) | ((ident == 1) & (c == 1)))
    def _():
        total = jnp.where(c >= 2, f[0, 0], 0.0)
        for k in range(2):
            high, low = halves(g[:, k].reshape(size, rows).T)
            total = total + (bf(low, yh[k]) + bf(high, yl[k]) + bf(high, yh[k]))
        out[0, 0] = jnp.where((ident == 1) & (c == 1) & (col > row), 0.0, total)

    @pl.when((ident <= jnp.minimum(c, 1)) & ((ident != c) | (c > 1)))
    def _():
        out[0, 0] = jnp.zeros((rows, size), jnp.float32)

    @pl.when((ident == 0) & (c == 0))
    def _():
        out[0, 0] = own_diag[:, pl.ds(pl.multiple_of(h * rows, rows), rows)].T


def last(place, gathered, y, matrix, own_diag):
    count, _, size, _ = matrix.shape
    part = 2
    rows = size // part
    tile = pl.BlockSpec((1, 1, rows, size), lambda a, h: (a, 0, h, 0))
    return pl.pallas_call(
        last_kernel,
        grid=(count, part),
        out_shape=jax.ShapeDtypeStruct(matrix.shape, jnp.float32),
        in_specs=[
            pl.BlockSpec(memory_space=pltpu.SMEM),
            pl.BlockSpec((8, 2, size // 8, rows), lambda a, h: (a, 0, 0, h)),
            pl.BlockSpec((2, size, size), lambda a, h: (0, 0, 0)),
            tile,
            pl.BlockSpec((size, size), lambda a, h: (0, 0)),
        ],
        out_specs=tile,
        scratch_shapes=[pltpu.VMEM((2, size, size), jnp.bfloat16)] * 2,
        compiler_params=pltpu.CompilerParams(vmem_limit_bytes=50 << 20),
        name="last",
    )(place, gathered, y, matrix, own_diag)


def send(v, pairs):
    return lax.ppermute(v, AXES, pairs)


def later(v, first):
    return v + jnp.minimum(jnp.abs(first[(0,) * first.ndim]), 0.0)


def broadcast(pieces, me, ahead=None, start=None):
    cols, ys, xs = range(N_COL), range(4), range(4)
    steps = []

    def wait(v):
        return v if ahead is None else later(v, ahead[len(steps)])

    held = jnp.where(me == ROOT, pieces, 0.0)
    if start is not None:
        held = later(held, start)
    for half in (4, 2, 1):
        pairs = [(at(0, 1, k, 0), at(0, 1, k + half, 0)) for k in range(0, N_COL, 2 * half)]
        held = wait(held)
        held = held[:half] + send(held[half:], pairs)
        steps.append(held)
    for pairs in (
        [(at(0, 1, k, 0), at(2, 1, k, 0)) for k in cols],
        [(at(y, 1, k, 0), at(y + 1, 1, k, 0)) for k in cols for y in (0, 2)],
        [(at(y, 1, k, 0), at(y, 1, k, 2)) for k in cols for y in ys],
        [(at(y, 1, k, x), at(y, 1, k, x + 1)) for k in cols for y in ys for x in (0, 2)],
    ):
        held = wait(held)
        held = held + send(held, pairs)
        steps.append(held)
    for bit in (4, 2, 1):
        pairs = [(at(y, 1, k, x), at(y, 1, k ^ bit, x)) for k in cols for y in ys for x in xs]
        held = wait(held)
        held = jnp.concatenate([held, send(held, pairs)])
        steps.append(held)
    pairs = [(at(y, 1, k, x), at(y, 0, k, x)) for k in cols for y in ys for x in xs]
    held = wait(held)
    other = send(held, [p for p in pairs if p[1] != OWNER])
    steps.append(other)
    return (held, other), steps


def body(matrix):
    mine = matrix[0, 0]
    size = mine.shape[0]
    r = lax.axis_index("row")
    z = lax.axis_index("col")
    c = lax.axis_index(("col", "depth"))
    me = lax.axis_index(AXES)
    owner = me == OWNER
    place = jnp.stack([c, r, owner.astype(jnp.int32), z]).astype(jnp.int32)
    flag = owner.astype(jnp.int32).reshape(1)

    inv0, packed0, up0, tick = factor(first_kernel, flag, mine)
    f10 = send(mine, [(ROOT, OWNER)])
    f11 = send(mine, [(dev(1, 1), OWNER)])

    step = size // 8
    after = later(mine, tick)
    got = []
    for k in range(8):
        pairs = [(dev(0, j), dev(j % 8, 8 * (j // 8) + k)) for j in range(1, N_BC)]
        pairs += [(dev(1, j), dev(j % 8, 8 * (j // 8) + (k + 4) % 8)) for j in range(1, N_BC)]
        got.append(send(after[k * step : (k + 1) * step], pairs))
    slot = c % 8
    first = sum(jnp.where(slot == k, got[k], 0.0) for k in range(8))
    second = sum(jnp.where(slot == (k + 4) % 8, got[k], 0.0) for k in range(8))
    shares, mine, f10, f11, packed0 = lax.optimization_barrier(
        (jnp.stack([first, second]), mine, f10, f11, packed0)
    )
    gathered = lax.all_gather(shares, ("col", "depth"))

    root0 = send(packed0, [(OWNER, ROOT)])
    _, packed1, _, _ = factor(second_kernel, flag, inv0, f10, f11)
    root1 = send(packed1, [(OWNER, ROOT)])
    cross, steps = broadcast(mine.reshape(8, step, size), me)
    got0, steps = broadcast(root0, me, steps)
    spread = steps[6]
    got1, _ = broadcast(root1, me, steps, spread)

    cs = range(2, N_BC)
    line = jnp.where(r < 2, mine, 0.0)
    line = line + send(mine, [(dev(a, j), dev(a + 2, j)) for j in cs for a in (0, 1)])
    line = line + send(mine, [(dev(a, j), dev(a + 6, j)) for j in cs for a in (0, 1)])
    line = later(line, spread)
    line = line + send(line, [(dev(a + 2, j), dev(a + 4, j)) for j in cs for a in (0, 1)])
    swap = send(line, [(dev(a, j), dev(a ^ 1, j)) for j in cs for a in range(8)])

    block = (size, size)
    own_cross = f10.reshape(8, step, size)
    x0, link, rest = multipliers(
        middle_kernel, [block] * 3, [block] * 2, place, line, swap, packed0, *got0, own_cross, *cross
    )
    (y,) = multipliers(tail_kernel, [(2,) + block], [block], place, packed1, *got1, x0, link, rest)
    return last(place, gathered, y, matrix, up0)


def solution(mesh):
    placed = P(None, "row", None, ("col", "depth"))
    return jax.shard_map(body, mesh=mesh, in_specs=(placed,), out_specs=placed, check_vma=False)
```

```python
import jax
import jax.numpy as jnp
from jax import lax
from jax.experimental import pallas as pl
from jax.experimental.pallas import tpu as pltpu
from jax.sharding import PartitionSpec as P

HI = lax.Precision.HIGHEST
NB = 32
OB = 128
AXES = ("row", "col", "depth")
N_ROW = 8
N_COL = 8
N_DEPTH = 4
N_BC = N_COL * N_DEPTH


def dev(r, c):
    return r * N_BC + c


def at(y, core, z, x):
    return dev(2 * y + core, z * N_DEPTH + x)


OWNER = dev(0, 0)
ROOT = dev(1, 0)


def dot(a, b, ca, cb, precision=HI):
    return lax.dot_general(
        a, b, (((ca,), (cb,)), ((), ())), precision=precision, preferred_element_type=jnp.float32
    )


def eliminate(rows, lane0):
    lanes = lax.broadcasted_iota(jnp.int32, (NB, OB), 1)
    subl = lax.broadcasted_iota(jnp.int32, (NB, OB), 0)
    ident = jnp.where(lanes == subl + lane0, jnp.float32(1.0), jnp.float32(0.0))
    groups = NB // 8

    def split(v):
        return [v[8 * g : 8 * g + 8] for g in range(groups)]

    cols = [
        split(jnp.broadcast_to(rows[:, lane0 + j : lane0 + j + 1], (NB, OB))) for j in range(NB)
    ]
    a = split(rows)
    x = split(ident)
    sub8 = lax.broadcasted_iota(jnp.int32, (8, OB), 0)
    for j in range(NB):
        gj, rj = j // 8, j % 8
        inv = lax.rsqrt(jnp.broadcast_to(cols[j][gj][rj : rj + 1], (8, OB)))
        lcol = [cols[j][g] * inv if g >= gj else None for g in range(groups)]
        ua = jnp.broadcast_to(a[gj][rj : rj + 1], (8, OB)) * inv
        ux = jnp.broadcast_to(x[gj][rj : rj + 1], (8, OB)) * inv
        mine = sub8 == rj
        if rj < 7:
            lself = jnp.where(sub8 > rj, lcol[gj], 0.0)
            a[gj] = jnp.where(mine, ua, a[gj] - lself * ua)
            x[gj] = jnp.where(mine, ux, x[gj] - lself * ux)
        else:
            a[gj] = jnp.where(mine, ua, a[gj])
            x[gj] = jnp.where(mine, ux, x[gj])
        for g in range(gj + 1, groups):
            a[g] = a[g] - lcol[g] * ua
            x[g] = x[g] - lcol[g] * ux
        for k in range(j + 1, NB):
            gk, rk = k // 8, k % 8
            s = jnp.broadcast_to(lcol[gk][rk : rk + 1], (8, OB))
            for g in range(gk, groups):
                cols[k][g] = cols[k][g] - lcol[g] * s
    return jnp.concatenate(a, axis=0), jnp.concatenate(x, axis=0)


def diag_block(w):
    n = OB // NB
    lanes = lax.broadcasted_iota(jnp.int32, (NB, OB), 1)
    subl = lax.broadcasted_iota(jnp.int32, (NB, OB), 0)
    wl = lax.broadcasted_iota(jnp.int32, (OB, OB), 1)
    ups = []
    done = []
    for i in range(n):
        lo = NB * i
        ua, ux = eliminate(w[lo : lo + NB], lo)
        inblk = (lanes >= lo) & (lanes < lo + NB)
        ups.append(jnp.where(lanes >= subl + lo, ua, 0.0))
        u = jnp.where(inblk, jnp.where(lanes <= subl + lo, ux, 0.0), ua)
        if i + 1 < n:
            um = jnp.where(lanes >= lo + NB, u, 0.0)
            w = jnp.where((wl >= lo) & (wl < lo + NB), 0.0, w) - dot(um, u, 0, 0)
        done.append(u)
        w = jnp.concatenate(done + [w[NB * (i + 1) :]] if i + 1 < n else done, axis=0)
    return w, jnp.concatenate(ups, axis=0)


def chol_body(inv_ref, up_ref, m):
    size = m.shape[0]
    nb = size // OB
    up_ref[...] = jnp.zeros((size, size), jnp.float32)
    il = lax.broadcasted_iota(jnp.int32, (OB, OB), 1)
    isb = lax.broadcasted_iota(jnp.int32, (OB, OB), 0)
    lane = lax.broadcasted_iota(jnp.int32, (OB, size), 1)

    def step(b, carry):
        off = pl.multiple_of(b * OB, OB)
        here = pl.ds(off, OB)
        inv, up = diag_block(m[here, here])
        inv = jnp.where(il <= isb, inv, 0.0)
        m[here, here] = jnp.where(il == isb, jnp.float32(1.0), jnp.float32(0.0))
        u = dot(inv, m[here, :], 1, 0)
        m[here, :] = u
        up_ref[here, :] = jnp.where(lane >= off + OB, u, 0.0)
        up_ref[here, here] = up

        def trail(k, c):
            there = pl.ds(pl.multiple_of(k * OB, OB), OB)
            prev = jnp.where((lane >= off) & (lane < off + OB), 0.0, m[there, :])
            m[there, :] = prev - dot(m[here, there], u, 0, 0)
            return c

        lax.fori_loop(b + 1, nb, trail, 0)
        return carry

    lax.fori_loop(0, nb, step, 0)
    row = lax.broadcasted_iota(jnp.int32, (size, size), 0)
    col = lax.broadcasted_iota(jnp.int32, (size, size), 1)
    inv_ref[...] = jnp.where(col <= row, m[...], 0.0)


def strips(size, move):
    for p in range(8):
        wide = OB * (p // 4 + 1)
        rest = size - wide
        top, bottom = NB * p, size - NB * (p + 1)
        move(p, 0, NB, slice(0, wide), top, slice(0, wide))
        move(p, 0, NB, slice(wide, size), bottom, slice(0, rest))
        for q in range(4):
            here = slice(OB * q, OB * (q + 1))
            move(p, NB, 8, here, bottom + 8 * q, slice(rest, rest + OB))


def pack(inv, packed):
    def move(p, row, rows, lanes, to_row, to_lanes):
        packed[p, row : row + rows, lanes] = inv[to_row : to_row + rows, to_lanes]

    strips(inv.shape[0], move)


def slot_of(place, p):
    v = lax.bitwise_xor(place[3], p)
    low, high = lax.bitwise_and(v, 1), lax.shift_right_logical(v, 2)
    return 4 * low + lax.bitwise_and(v, 2) + high


def unpack(packed, inv, slots, first=0):
    def move(p, row, rows, lanes, to_row, to_lanes):
        here = slice(first + row, first + row + rows)
        inv[to_row : to_row + rows, to_lanes] = packed[slots[p], here, lanes]

    inv[...] = jnp.zeros(inv.shape, jnp.float32)
    strips(inv.shape[0], move)


def middle_kernel(place, line, swap, own_cross, own0, one, zero, x0, link, rest, inv, w1):
    c = place[0]
    even = lax.rem(place[1], 2) == 0
    size = inv.shape[0]
    owner = place[2] == 1
    on_one = lax.rem(place[1], 2) == 1
    part = size // 8
    slots = [slot_of(place, p) for p in range(8)]

    def take(ref):
        unpack(ref, inv, slots, part)
        for p in range(8):
            rest[part * p : part * (p + 1)] = ref[slots[p], :part]

    @pl.when(owner)
    def _():
        unpack(own0, inv, list(range(8)))
        rest[...] = own_cross[...]

    @pl.when(on_one)
    def _():
        take(one)

    @pl.when(jnp.logical_not(owner | on_one))
    def _():
        take(zero)

    def keep(a, b):
        x0[...] = a[...]
        w1[...] = b[...]

    @pl.when(even)
    def _():
        keep(line, swap)

    @pl.when(jnp.logical_not(even))
    def _():
        keep(swap, line)

    il = lax.broadcasted_iota(jnp.int32, (size, size), 1)
    isb = lax.broadcasted_iota(jnp.int32, (size, size), 0)
    eye = jnp.where(il == isb, jnp.float32(1.0), jnp.float32(0.0))
    q0 = dot(inv[...], x0[...], 1, 0)
    q0 = jnp.where(c == 0, -eye, jnp.where(c == 1, 0.0, q0))
    x0[...] = dot(inv[...], q0, 0, 0)
    link[...] = dot(inv[...], dot(inv[...], rest[...], 1, 1), 0, 0)
    rest[...] = w1[...] - dot(rest[...], x0[...], 1, 0)


def tail_kernel(place, zero, one, x0, link, rest, y, inv):
    c = place[0]
    size = inv.shape[0]
    slots = [slot_of(place, p) for p in range(8)]

    @pl.when(lax.rem(place[1], 2) == 0)
    def _():
        unpack(zero, inv, slots)

    @pl.when(lax.rem(place[1], 2) == 1)
    def _():
        unpack(one, inv, slots)

    il = lax.broadcasted_iota(jnp.int32, (size, size), 1)
    isb = lax.broadcasted_iota(jnp.int32, (size, size), 0)
    eye = jnp.where(il == isb, jnp.float32(1.0), jnp.float32(0.0))
    q1 = dot(inv[...], rest[...], 1, 0)
    q1 = jnp.where(c == 0, 0.0, jnp.where(c == 1, -eye, q1))
    y1 = -dot(inv[...], q1, 0, 0)
    y[1] = y1
    y[0] = -x0[...] - dot(link[...], y1, 1, 0)


def multipliers(kernel, outs, scratch, place, *ins):
    vm = pl.BlockSpec(memory_space=pltpu.VMEM)
    return pl.pallas_call(
        kernel,
        out_shape=tuple(jax.ShapeDtypeStruct(o, jnp.float32) for o in outs),
        in_specs=[pl.BlockSpec(memory_space=pltpu.SMEM)] + [vm] * len(ins),
        out_specs=(vm,) * len(outs),
        scratch_shapes=[pltpu.VMEM(o, jnp.float32) for o in scratch],
        compiler_params=pltpu.CompilerParams(vmem_limit_bytes=50 << 20),
        name=kernel.__name__,
    )(place, *ins)


def first_kernel(flag, f00, inv, packed, up, tick, m):
    tick[...] = jnp.zeros(tick.shape, jnp.float32)

    @pl.when(flag[0] == 1)
    def _():
        m[...] = f00[...]
        chol_body(inv, up, m)
        pack(inv, packed)


def second_kernel(flag, inv0, f10, f11, inv, packed, up, tick, m):
    tick[...] = jnp.zeros(tick.shape, jnp.float32)

    @pl.when(flag[0] == 1)
    def _():
        q = dot(inv0[...], f10[...], 1, 1)
        m[...] = f11[...] - dot(q, q, 0, 0)
        chol_body(inv, up, m)
        pack(inv, packed)


def factor(kernel, flag, *ins):
    size = ins[0].shape[0]
    out = jax.ShapeDtypeStruct((size, size), jnp.float32)
    packed = jax.ShapeDtypeStruct((8, NB + 8, size), jnp.float32)
    vm = pl.BlockSpec(memory_space=pltpu.VMEM)
    return pl.pallas_call(
        kernel,
        out_shape=(out, packed, out, jax.ShapeDtypeStruct((8, OB), jnp.float32)),
        in_specs=[pl.BlockSpec(memory_space=pltpu.SMEM)] + [vm] * len(ins),
        out_specs=(vm, vm, vm, vm),
        scratch_shapes=[pltpu.VMEM((size, size), jnp.float32)],
        compiler_params=pltpu.CompilerParams(vmem_limit_bytes=32 << 20),
        name=kernel.__name__,
    )(flag, *ins)


def halves(v):
    high = v.astype(jnp.bfloat16)
    return high, (v - high.astype(jnp.float32)).astype(jnp.bfloat16)


def last_kernel(place, g, y, f, own_diag, out, yh, yl):
    a = pl.program_id(0)
    h = pl.program_id(1)
    c = place[0]
    ident = a * N_ROW + place[1]
    size = y.shape[1]
    half = size // 2

    @pl.when((a == 0) & (h == 0))
    def _():
        for k, ref in enumerate(halves(y[0])):
            (yh, yl)[k][0] = ref
        for k in range(2):
            for n, ref in enumerate(halves(y[1, half * k : half * (k + 1)])):
                (yh, yl)[n][1, half * (1 - k) : half * (2 - k)] = ref

    rows = out.shape[2]

    def bf(p, q):
        return jnp.dot(p, q, preferred_element_type=jnp.float32)

    row = lax.broadcasted_iota(jnp.int32, (rows, size), 0) + h * rows
    col = lax.broadcasted_iota(jnp.int32, (rows, size), 1)

    @pl.when((ident > jnp.minimum(c, 1)) | ((ident == 1) & (c == 1)))
    def _():
        total = jnp.where(c >= 2, f[0, 0], 0.0)
        for k in range(2):
            high, low = halves(g[:, k].reshape(size, rows).T)
            total = total + (bf(low, yh[k]) + bf(high, yl[k]) + bf(high, yh[k]))
        out[0, 0] = jnp.where((ident == 1) & (c == 1) & (col > row), 0.0, total)

    @pl.when((ident <= jnp.minimum(c, 1)) & ((ident != c) | (c > 1)))
    def _():
        out[0, 0] = jnp.zeros((rows, size), jnp.float32)

    @pl.when((ident == 0) & (c == 0))
    def _():
        out[0, 0] = own_diag[:, pl.ds(pl.multiple_of(h * rows, rows), rows)].T


def last(place, gathered, y, matrix, own_diag):
    count, _, size, _ = matrix.shape
    part = 2
    rows = size // part
    tile = pl.BlockSpec((1, 1, rows, size), lambda a, h: (a, 0, h, 0))
    return pl.pallas_call(
        last_kernel,
        grid=(count, part),
        out_shape=jax.ShapeDtypeStruct(matrix.shape, jnp.float32),
        in_specs=[
            pl.BlockSpec(memory_space=pltpu.SMEM),
            pl.BlockSpec((8, 2, size // 8, rows), lambda a, h: (a, 0, 0, h)),
            pl.BlockSpec((2, size, size), lambda a, h: (0, 0, 0)),
            tile,
            pl.BlockSpec((size, size), lambda a, h: (0, 0)),
        ],
        out_specs=tile,
        scratch_shapes=[pltpu.VMEM((2, size, size), jnp.bfloat16)] * 2,
        compiler_params=pltpu.CompilerParams(vmem_limit_bytes=50 << 20),
        name="last",
    )(place, gathered, y, matrix, own_diag)


def send(v, pairs):
    return lax.ppermute(v, AXES, pairs)


def later(v, first):
    return v + jnp.minimum(jnp.abs(first[(0,) * first.ndim]), 0.0)


def broadcast(pieces, me, core, skip=()):
    cols, ys, xs = range(N_COL), range(4), range(4)
    held = jnp.where(me == at(0, core, 0, 0), pieces, 0.0)
    for half in (4, 2, 1):
        pairs = [(at(0, core, k, 0), at(0, core, k + half, 0)) for k in range(0, N_COL, 2 * half)]
        held = held[:half] + send(held[half:], pairs)
    for pairs in (
        [(at(0, core, k, 0), at(2, core, k, 0)) for k in cols],
        [(at(y, core, k, 0), at(y + 1, core, k, 0)) for k in cols for y in (0, 2)],
        [(at(y, core, k, 0), at(y, core, k, 2)) for k in cols for y in ys],
        [(at(y, core, k, x), at(y, core, k, x + 1)) for k in cols for y in ys for x in (0, 2)],
    ):
        held = held + send(held, pairs)
    spread = held
    for bit in (4, 2, 1):
        pairs = [(at(y, core, k, x), at(y, core, k ^ bit, x)) for k in cols for y in ys for x in xs]
        held = jnp.concatenate([held, send(held, pairs)])
    pairs = [(at(y, core, k, x), at(y, 1 - core, k, x)) for k in cols for y in ys for x in xs]
    other = send(held, [p for p in pairs if p[1] not in skip])
    return (held, other), spread


def body(matrix):
    mine = matrix[0, 0]
    size = mine.shape[0]
    r = lax.axis_index("row")
    z = lax.axis_index("col")
    c = lax.axis_index(("col", "depth"))
    me = lax.axis_index(AXES)
    owner = me == OWNER
    place = jnp.stack([c, r, owner.astype(jnp.int32), z]).astype(jnp.int32)
    flag = owner.astype(jnp.int32).reshape(1)

    inv0, packed0, up0, tick = factor(first_kernel, flag, mine)
    f10 = send(mine, [(ROOT, OWNER)])
    f11 = send(mine, [(dev(1, 1), OWNER)])

    step = size // 8
    after = later(mine, tick)
    got = []
    for k in range(8):
        pairs = [(dev(0, j), dev(j % 8, 8 * (j // 8) + k)) for j in range(1, N_BC)]
        pairs += [(dev(1, j), dev(j % 8, 8 * (j // 8) + (k + 4) % 8)) for j in range(1, N_BC)]
        got.append(send(after[k * step : (k + 1) * step], pairs))
    slot = c % 8
    first = sum(jnp.where(slot == k, got[k], 0.0) for k in range(8))
    second = sum(jnp.where(slot == (k + 4) % 8, got[k], 0.0) for k in range(8))
    shares, mine, f10, f11, packed0 = lax.optimization_barrier(
        (jnp.stack([first, second]), mine, f10, f11, packed0)
    )
    gathered = lax.all_gather(shares, ("col", "depth"))

    root0 = send(packed0, [(OWNER, ROOT)])
    _, packed1, _, tick = factor(second_kernel, flag, inv0, f10, f11)
    cross = later(mine, tick).reshape(8, step, size)
    first, spread = broadcast(jnp.concatenate([cross, root0], axis=1), me, 1, (OWNER,))
    second, _ = broadcast(packed1, me, 0)

    cs = range(2, N_BC)
    line = jnp.where(r < 2, mine, 0.0)
    line = line + send(line, [(dev(a, j), dev(a + 2, j)) for j in cs for a in (0, 1)])
    line = later(line, spread)
    hops = [(0, 6), (1, 7), (2, 4), (3, 5)]
    line = line + send(line, [(dev(a, j), dev(b, j)) for j in cs for a, b in hops])
    swap = send(line, [(dev(a, j), dev(a ^ 1, j)) for j in cs for a in range(8)])

    block = (size, size)
    x0, link, rest = multipliers(
        middle_kernel, [block] * 3, [block] * 2, place, line, swap, f10, packed0, *first
    )
    (y,) = multipliers(tail_kernel, [(2,) + block], [block], place, *second, x0, link, rest)
    return last(place, gathered, y, matrix, up0)


def solution(mesh):
    placed = P(None, "row", None, ("col", "depth"))
    return jax.shard_map(body, mesh=mesh, in_specs=(placed,), out_specs=placed, check_vma=False)
```

```python
import jax
import jax.numpy as jnp
from jax import lax
from jax.experimental import pallas as pl
from jax.experimental.pallas import tpu as pltpu
from jax.sharding import PartitionSpec as P

HI = lax.Precision.HIGHEST
NB = 32
OB = 128
AXES = ("row", "col", "depth")
N_ROW = 8
N_COL = 8
N_DEPTH = 4
N_BC = N_COL * N_DEPTH


def dev(r, c):
    return r * N_BC + c


def at(y, core, z, x):
    return dev(2 * y + core, z * N_DEPTH + x)


OWNER = dev(0, 0)
ROOT = dev(1, 0)


def dot(a, b, ca, cb, precision=HI):
    return lax.dot_general(
        a, b, (((ca,), (cb,)), ((), ())), precision=precision, preferred_element_type=jnp.float32
    )


def eliminate(rows, lane0):
    lanes = lax.broadcasted_iota(jnp.int32, (NB, OB), 1)
    subl = lax.broadcasted_iota(jnp.int32, (NB, OB), 0)
    ident = jnp.where(lanes == subl + lane0, jnp.float32(1.0), jnp.float32(0.0))
    groups = NB // 8

    def split(v):
        return [v[8 * g : 8 * g + 8] for g in range(groups)]

    cols = [
        split(jnp.broadcast_to(rows[:, lane0 + j : lane0 + j + 1], (NB, OB))) for j in range(NB)
    ]
    a = split(rows)
    x = split(ident)
    sub8 = lax.broadcasted_iota(jnp.int32, (8, OB), 0)
    for j in range(NB):
        gj, rj = j // 8, j % 8
        inv = lax.rsqrt(jnp.broadcast_to(cols[j][gj][rj : rj + 1], (8, OB)))
        lcol = [cols[j][g] * inv if g >= gj else None for g in range(groups)]
        ua = jnp.broadcast_to(a[gj][rj : rj + 1], (8, OB)) * inv
        ux = jnp.broadcast_to(x[gj][rj : rj + 1], (8, OB)) * inv
        mine = sub8 == rj
        if rj < 7:
            lself = jnp.where(sub8 > rj, lcol[gj], 0.0)
            a[gj] = jnp.where(mine, ua, a[gj] - lself * ua)
            x[gj] = jnp.where(mine, ux, x[gj] - lself * ux)
        else:
            a[gj] = jnp.where(mine, ua, a[gj])
            x[gj] = jnp.where(mine, ux, x[gj])
        for g in range(gj + 1, groups):
            a[g] = a[g] - lcol[g] * ua
            x[g] = x[g] - lcol[g] * ux
        for k in range(j + 1, NB):
            gk, rk = k // 8, k % 8
            s = jnp.broadcast_to(lcol[gk][rk : rk + 1], (8, OB))
            for g in range(gk, groups):
                cols[k][g] = cols[k][g] - lcol[g] * s
    return jnp.concatenate(a, axis=0), jnp.concatenate(x, axis=0)


def diag_block(w):
    n = OB // NB
    lanes = lax.broadcasted_iota(jnp.int32, (NB, OB), 1)
    subl = lax.broadcasted_iota(jnp.int32, (NB, OB), 0)
    wl = lax.broadcasted_iota(jnp.int32, (OB, OB), 1)
    ups = []
    done = []
    for i in range(n):
        lo = NB * i
        ua, ux = eliminate(w[lo : lo + NB], lo)
        inblk = (lanes >= lo) & (lanes < lo + NB)
        ups.append(jnp.where(lanes >= subl + lo, ua, 0.0))
        u = jnp.where(inblk, jnp.where(lanes <= subl + lo, ux, 0.0), ua)
        if i + 1 < n:
            um = jnp.where(lanes >= lo + NB, u, 0.0)
            w = jnp.where((wl >= lo) & (wl < lo + NB), 0.0, w) - dot(um, u, 0, 0)
        done.append(u)
        w = jnp.concatenate(done + [w[NB * (i + 1) :]] if i + 1 < n else done, axis=0)
    return w, jnp.concatenate(ups, axis=0)


def chol_body(inv_ref, up_ref, m):
    size = m.shape[0]
    nb = size // OB
    up_ref[...] = jnp.zeros((size, size), jnp.float32)
    il = lax.broadcasted_iota(jnp.int32, (OB, OB), 1)
    isb = lax.broadcasted_iota(jnp.int32, (OB, OB), 0)
    lane = lax.broadcasted_iota(jnp.int32, (OB, size), 1)

    def step(b, carry):
        off = pl.multiple_of(b * OB, OB)
        here = pl.ds(off, OB)
        inv, up = diag_block(m[here, here])
        inv = jnp.where(il <= isb, inv, 0.0)
        m[here, here] = jnp.where(il == isb, jnp.float32(1.0), jnp.float32(0.0))
        u = dot(inv, m[here, :], 1, 0)
        m[here, :] = u
        up_ref[here, :] = jnp.where(lane >= off + OB, u, 0.0)
        up_ref[here, here] = up

        def trail(k, c):
            there = pl.ds(pl.multiple_of(k * OB, OB), OB)
            prev = jnp.where((lane >= off) & (lane < off + OB), 0.0, m[there, :])
            m[there, :] = prev - dot(m[here, there], u, 0, 0)
            return c

        lax.fori_loop(b + 1, nb, trail, 0)
        return carry

    lax.fori_loop(0, nb, step, 0)
    row = lax.broadcasted_iota(jnp.int32, (size, size), 0)
    col = lax.broadcasted_iota(jnp.int32, (size, size), 1)
    inv_ref[...] = jnp.where(col <= row, m[...], 0.0)


def strips(size, move):
    for p in range(8):
        wide = OB * (p // 4 + 1)
        rest = size - wide
        top, bottom = NB * p, size - NB * (p + 1)
        move(p, 0, NB, slice(0, wide), top, slice(0, wide))
        move(p, 0, NB, slice(wide, size), bottom, slice(0, rest))
        for q in range(4):
            here = slice(OB * q, OB * (q + 1))
            move(p, NB, 8, here, bottom + 8 * q, slice(rest, rest + OB))


def pack(inv, packed):
    def move(p, row, rows, lanes, to_row, to_lanes):
        packed[p, row : row + rows, lanes] = inv[to_row : to_row + rows, to_lanes]

    strips(inv.shape[0], move)


def slot_of(place, p):
    v = lax.bitwise_xor(place[3], p)
    low, high = lax.bitwise_and(v, 1), lax.shift_right_logical(v, 2)
    return 4 * low + lax.bitwise_and(v, 2) + high


def unpack(packed, inv, slots):
    def move(p, row, rows, lanes, to_row, to_lanes):
        inv[to_row : to_row + rows, to_lanes] = packed[slots[p], row : row + rows, lanes]

    inv[...] = jnp.zeros(inv.shape, jnp.float32)
    strips(inv.shape[0], move)


def take_inverse(place, own, one, zero, inv):
    slots = [slot_of(place, p) for p in range(8)]
    owner = place[2] == 1
    on_one = lax.rem(place[1], 2) == 1

    @pl.when(owner)
    def _():
        unpack(own, inv, list(range(8)))

    @pl.when(on_one)
    def _():
        unpack(one, inv, slots)

    @pl.when(jnp.logical_not(owner | on_one))
    def _():
        unpack(zero, inv, slots)


def middle_kernel(
    place, line, swap, own0, one0, zero0, zero_cross, one_cross, x0, link, rest, inv, w1
):
    c = place[0]
    even = lax.rem(place[1], 2) == 0
    size = inv.shape[0]
    part = size // 8
    take_inverse(place, own0, one0, zero0, inv)

    def keep_cross(ref):
        for p in range(8):
            rest[part * p : part * (p + 1)] = ref[slot_of(place, p)]

    @pl.when(even)
    def _():
        keep_cross(zero_cross)

    @pl.when(jnp.logical_not(even))
    def _():
        keep_cross(one_cross)

    def keep(a, b):
        x0[...] = a[...]
        w1[...] = b[...]

    @pl.when(even)
    def _():
        keep(line, swap)

    @pl.when(jnp.logical_not(even))
    def _():
        keep(swap, line)

    il = lax.broadcasted_iota(jnp.int32, (size, size), 1)
    isb = lax.broadcasted_iota(jnp.int32, (size, size), 0)
    eye = jnp.where(il == isb, jnp.float32(1.0), jnp.float32(0.0))
    q0 = dot(inv[...], x0[...], 1, 0)
    q0 = jnp.where(c == 0, -eye, jnp.where(c == 1, 0.0, q0))
    x0[...] = dot(inv[...], q0, 0, 0)
    link[...] = dot(inv[...], dot(inv[...], rest[...], 1, 0), 0, 0)
    rest[...] = w1[...] - dot(rest[...], x0[...], 0, 0)


def tail_kernel(place, own1, one1, zero1, x0, link, rest, y, inv):
    c = place[0]
    size = inv.shape[0]
    take_inverse(place, own1, one1, zero1, inv)
    il = lax.broadcasted_iota(jnp.int32, (size, size), 1)
    isb = lax.broadcasted_iota(jnp.int32, (size, size), 0)
    eye = jnp.where(il == isb, jnp.float32(1.0), jnp.float32(0.0))
    q1 = dot(inv[...], rest[...], 1, 0)
    q1 = jnp.where(c == 0, 0.0, jnp.where(c == 1, -eye, q1))
    y1 = -dot(inv[...], q1, 0, 0)
    y[1] = y1
    y[0] = -x0[...] - dot(link[...], y1, 1, 0)


def multipliers(kernel, outs, scratch, place, *ins):
    vm = pl.BlockSpec(memory_space=pltpu.VMEM)
    return pl.pallas_call(
        kernel,
        out_shape=tuple(jax.ShapeDtypeStruct(o, jnp.float32) for o in outs),
        in_specs=[pl.BlockSpec(memory_space=pltpu.SMEM)] + [vm] * len(ins),
        out_specs=(vm,) * len(outs),
        scratch_shapes=[pltpu.VMEM(o, jnp.float32) for o in scratch],
        compiler_params=pltpu.CompilerParams(vmem_limit_bytes=50 << 20),
        name=kernel.__name__,
    )(place, *ins)


def first_kernel(flag, f00, inv, packed, up, tick, m):
    tick[...] = jnp.zeros(tick.shape, jnp.float32)

    @pl.when(flag[0] == 1)
    def _():
        m[...] = f00[...]
        chol_body(inv, up, m)
        pack(inv, packed)


def second_kernel(flag, inv0, f10, f11, inv, packed, up, tick, m):
    tick[...] = jnp.zeros(tick.shape, jnp.float32)

    @pl.when(flag[0] == 1)
    def _():
        q = dot(inv0[...], f10[...], 1, 1)
        m[...] = f11[...] - dot(q, q, 0, 0)
        chol_body(inv, up, m)
        pack(inv, packed)


def factor(kernel, flag, *ins):
    size = ins[0].shape[0]
    out = jax.ShapeDtypeStruct((size, size), jnp.float32)
    packed = jax.ShapeDtypeStruct((8, NB + 8, size), jnp.float32)
    vm = pl.BlockSpec(memory_space=pltpu.VMEM)
    return pl.pallas_call(
        kernel,
        out_shape=(out, packed, out, jax.ShapeDtypeStruct((8, OB), jnp.float32)),
        in_specs=[pl.BlockSpec(memory_space=pltpu.SMEM)] + [vm] * len(ins),
        out_specs=(vm, vm, vm, vm),
        scratch_shapes=[pltpu.VMEM((size, size), jnp.float32)],
        compiler_params=pltpu.CompilerParams(vmem_limit_bytes=32 << 20),
        name=kernel.__name__,
    )(flag, *ins)


def halves(v):
    high = v.astype(jnp.bfloat16)
    return high, (v - high.astype(jnp.float32)).astype(jnp.bfloat16)


def last_kernel(place, g, y, f, own_diag, out, yh, yl):
    a = pl.program_id(0)
    h = pl.program_id(1)
    c = place[0]
    ident = a * N_ROW + place[1]
    size = y.shape[1]
    half = size // 2

    @pl.when((a == 0) & (h == 0))
    def _():
        for k, ref in enumerate(halves(y[0])):
            (yh, yl)[k][0] = ref
        for k in range(2):
            for n, ref in enumerate(halves(y[1, half * k : half * (k + 1)])):
                (yh, yl)[n][1, half * (1 - k) : half * (2 - k)] = ref

    rows = out.shape[2]

    def bf(p, q):
        return jnp.dot(p, q, preferred_element_type=jnp.float32)

    row = lax.broadcasted_iota(jnp.int32, (rows, size), 0) + h * rows
    col = lax.broadcasted_iota(jnp.int32, (rows, size), 1)

    @pl.when((ident > jnp.minimum(c, 1)) | ((ident == 1) & (c == 1)))
    def _():
        total = jnp.where(c >= 2, f[0, 0], 0.0)
        for k in range(2):
            high, low = halves(g[:, k].reshape(size, rows).T)
            total = total + (bf(low, yh[k]) + bf(high, yl[k]) + bf(high, yh[k]))
        out[0, 0] = jnp.where((ident == 1) & (c == 1) & (col > row), 0.0, total)

    @pl.when((ident <= jnp.minimum(c, 1)) & ((ident != c) | (c > 1)))
    def _():
        out[0, 0] = jnp.zeros((rows, size), jnp.float32)

    @pl.when((ident == 0) & (c == 0))
    def _():
        out[0, 0] = own_diag[:, pl.ds(pl.multiple_of(h * rows, rows), rows)].T


def last(place, gathered, y, matrix, own_diag):
    count, _, size, _ = matrix.shape
    part = 2
    rows = size // part
    tile = pl.BlockSpec((1, 1, rows, size), lambda a, h: (a, 0, h, 0))
    return pl.pallas_call(
        last_kernel,
        grid=(count, part),
        out_shape=jax.ShapeDtypeStruct(matrix.shape, jnp.float32),
        in_specs=[
            pl.BlockSpec(memory_space=pltpu.SMEM),
            pl.BlockSpec((8, 2, size // 8, rows), lambda a, h: (a, 0, 0, h)),
            pl.BlockSpec((2, size, size), lambda a, h: (0, 0, 0)),
            tile,
            pl.BlockSpec((size, size), lambda a, h: (0, 0)),
        ],
        out_specs=tile,
        scratch_shapes=[pltpu.VMEM((2, size, size), jnp.bfloat16)] * 2,
        compiler_params=pltpu.CompilerParams(vmem_limit_bytes=50 << 20),
        name="last",
    )(place, gathered, y, matrix, own_diag)


def send(v, pairs):
    return lax.ppermute(v, AXES, pairs)


def later(v, first):
    return v + jnp.minimum(jnp.abs(first[(0,) * first.ndim]), 0.0)


def broadcast(pieces, me, core, x0, skip=(), ahead=None, start=None):
    cols, ys, xs = range(N_COL), range(4), range(4)
    steps = []

    def wait(v):
        return v if ahead is None else later(v, ahead[len(steps)])

    held = jnp.where(me == at(0, core, 0, x0), pieces, 0.0)
    if start is not None:
        held = later(held, start)
    for half in (4, 2, 1):
        pairs = [(at(0, core, k, x0), at(0, core, k + half, x0)) for k in range(0, N_COL, 2 * half)]
        held = wait(held)
        held = held[:half] + send(held[half:], pairs)
        steps.append(held)
    x1, x2, x3 = x0 ^ 1, x0 ^ 2, x0 ^ 3
    for pairs in (
        [(at(0, core, k, x0), at(2, core, k, x0)) for k in cols],
        [(at(y, core, k, x0), at(y + 1, core, k, x0)) for k in cols for y in (0, 2)],
        [(at(y, core, k, x0), at(y, core, k, x2)) for k in cols for y in ys],
        [
            (at(y, core, k, a), at(y, core, k, b))
            for k in cols
            for y in ys
            for a, b in ((x0, x1), (x2, x3))
        ],
    ):
        held = wait(held)
        held = held + send(held, pairs)
        steps.append(held)
    for bit in (4, 2, 1):
        pairs = [(at(y, core, k, x), at(y, core, k ^ bit, x)) for k in cols for y in ys for x in xs]
        held = wait(held)
        held = jnp.concatenate([held, send(held, pairs)])
        steps.append(held)
    pairs = [(at(y, core, k, x), at(y, 1 - core, k, x)) for k in cols for y in ys for x in xs]
    held = wait(held)
    other = send(held, [p for p in pairs if p[1] not in skip])
    steps.append(other)
    return (held, other), steps


def body(matrix):
    mine = matrix[0, 0]
    size = mine.shape[0]
    r = lax.axis_index("row")
    z = lax.axis_index("col")
    c = lax.axis_index(("col", "depth"))
    me = lax.axis_index(AXES)
    owner = me == OWNER
    place = jnp.stack([c, r, owner.astype(jnp.int32), z]).astype(jnp.int32)
    flag = owner.astype(jnp.int32).reshape(1)

    inv0, packed0, up0, tick = factor(first_kernel, flag, mine)
    f10 = send(mine, [(ROOT, OWNER)])
    f11 = send(mine, [(dev(1, 1), OWNER)])

    step = size // 8
    after = later(mine, tick)
    got = []
    for k in range(8):
        pairs = [(dev(0, j), dev(j % 8, 8 * (j // 8) + k)) for j in range(1, N_BC)]
        pairs += [(dev(1, j), dev(j % 8, 8 * (j // 8) + (k + 4) % 8)) for j in range(1, N_BC)]
        got.append(send(after[k * step : (k + 1) * step], pairs))
    slot = c % 8
    first = sum(jnp.where(slot == k, got[k], 0.0) for k in range(8))
    second = sum(jnp.where(slot == (k + 4) % 8, got[k], 0.0) for k in range(8))
    shares, mine, f10, f11, packed0 = lax.optimization_barrier(
        (jnp.stack([first, second]), mine, f10, f11, packed0)
    )
    gathered = lax.all_gather(shares, ("col", "depth"))

    root0 = send(packed0, [(OWNER, ROOT)])
    _, packed1, _, tick = factor(second_kernel, flag, inv0, f10, f11)
    root1 = send(packed1, [(OWNER, ROOT)])
    cross, _ = broadcast(later(mine, tick).reshape(8, step, size), me, 0, 1)
    first, steps = broadcast(root0, me, 1, 0, (OWNER,))
    spread = steps[6]
    second, _ = broadcast(root1, me, 1, 0, (OWNER,), steps, spread)

    cs = range(2, N_BC)
    line = jnp.where(r < 2, mine, 0.0)
    line = line + send(line, [(dev(a, j), dev(a + 2, j)) for j in cs for a in (0, 1)])
    line = later(line, spread)
    hops = [(0, 6), (1, 7), (2, 4), (3, 5)]
    line = line + send(line, [(dev(a, j), dev(b, j)) for j in cs for a, b in hops])
    swap = send(line, [(dev(a, j), dev(a ^ 1, j)) for j in cs for a in range(8)])

    block = (size, size)
    x0, link, rest = multipliers(
        middle_kernel, [block] * 3, [block] * 2, place, line, swap, packed0, *first, *cross
    )
    (y,) = multipliers(
        tail_kernel, [(2,) + block], [block], place, packed1, *second, x0, link, rest
    )
    return last(place, gathered, y, matrix, up0)


def solution(mesh):
    placed = P(None, "row", None, ("col", "depth"))
    return jax.shard_map(body, mesh=mesh, in_specs=(placed,), out_specs=placed, check_vma=False)
```

```python
import jax
import jax.numpy as jnp
from jax import lax
from jax.experimental import pallas as pl
from jax.experimental.pallas import tpu as pltpu
from jax.sharding import PartitionSpec as P

HI = lax.Precision.HIGHEST
NB = 32
OB = 128
AXES = ("row", "col", "depth")
N_ROW = 8
N_COL = 8
N_DEPTH = 4
N_BC = N_COL * N_DEPTH


def dev(r, c):
    return r * N_BC + c


def at(y, core, z, x):
    return dev(2 * y + core, z * N_DEPTH + x)


OWNER = dev(0, 0)
ROOT = dev(1, 0)


def dot(a, b, ca, cb, precision=HI):
    return lax.dot_general(
        a, b, (((ca,), (cb,)), ((), ())), precision=precision, preferred_element_type=jnp.float32
    )


def eliminate(rows, lane0):
    lanes = lax.broadcasted_iota(jnp.int32, (NB, OB), 1)
    subl = lax.broadcasted_iota(jnp.int32, (NB, OB), 0)
    ident = jnp.where(lanes == subl + lane0, jnp.float32(1.0), jnp.float32(0.0))
    groups = NB // 8

    def split(v):
        return [v[8 * g : 8 * g + 8] for g in range(groups)]

    cols = [
        split(jnp.broadcast_to(rows[:, lane0 + j : lane0 + j + 1], (NB, OB))) for j in range(NB)
    ]
    a = split(rows)
    x = split(ident)
    sub8 = lax.broadcasted_iota(jnp.int32, (8, OB), 0)
    for j in range(NB):
        gj, rj = j // 8, j % 8
        inv = lax.rsqrt(jnp.broadcast_to(cols[j][gj][rj : rj + 1], (8, OB)))
        lcol = [cols[j][g] * inv if g >= gj else None for g in range(groups)]
        ua = jnp.broadcast_to(a[gj][rj : rj + 1], (8, OB)) * inv
        ux = jnp.broadcast_to(x[gj][rj : rj + 1], (8, OB)) * inv
        mine = sub8 == rj
        if rj < 7:
            lself = jnp.where(sub8 > rj, lcol[gj], 0.0)
            a[gj] = jnp.where(mine, ua, a[gj] - lself * ua)
            x[gj] = jnp.where(mine, ux, x[gj] - lself * ux)
        else:
            a[gj] = jnp.where(mine, ua, a[gj])
            x[gj] = jnp.where(mine, ux, x[gj])
        for g in range(gj + 1, groups):
            a[g] = a[g] - lcol[g] * ua
            x[g] = x[g] - lcol[g] * ux
        for k in range(j + 1, NB):
            gk, rk = k // 8, k % 8
            s = jnp.broadcast_to(lcol[gk][rk : rk + 1], (8, OB))
            for g in range(gk, groups):
                cols[k][g] = cols[k][g] - lcol[g] * s
    return jnp.concatenate(a, axis=0), jnp.concatenate(x, axis=0)


def diag_block(w):
    n = OB // NB
    lanes = lax.broadcasted_iota(jnp.int32, (NB, OB), 1)
    subl = lax.broadcasted_iota(jnp.int32, (NB, OB), 0)
    wl = lax.broadcasted_iota(jnp.int32, (OB, OB), 1)
    ups = []
    done = []
    for i in range(n):
        lo = NB * i
        ua, ux = eliminate(w[lo : lo + NB], lo)
        inblk = (lanes >= lo) & (lanes < lo + NB)
        ups.append(jnp.where(lanes >= subl + lo, ua, 0.0))
        u = jnp.where(inblk, jnp.where(lanes <= subl + lo, ux, 0.0), ua)
        if i + 1 < n:
            um = jnp.where(lanes >= lo + NB, u, 0.0)
            w = jnp.where((wl >= lo) & (wl < lo + NB), 0.0, w) - dot(um, u, 0, 0)
        done.append(u)
        w = jnp.concatenate(done + [w[NB * (i + 1) :]] if i + 1 < n else done, axis=0)
    return w, jnp.concatenate(ups, axis=0)


def chol_body(inv_ref, up_ref, m):
    size = m.shape[0]
    nb = size // OB
    up_ref[...] = jnp.zeros((size, size), jnp.float32)
    il = lax.broadcasted_iota(jnp.int32, (OB, OB), 1)
    isb = lax.broadcasted_iota(jnp.int32, (OB, OB), 0)
    lane = lax.broadcasted_iota(jnp.int32, (OB, size), 1)

    def step(b, carry):
        off = pl.multiple_of(b * OB, OB)
        here = pl.ds(off, OB)
        inv, up = diag_block(m[here, here])
        inv = jnp.where(il <= isb, inv, 0.0)
        m[here, here] = jnp.where(il == isb, jnp.float32(1.0), jnp.float32(0.0))
        u = dot(inv, m[here, :], 1, 0)
        m[here, :] = u
        up_ref[here, :] = jnp.where(lane >= off + OB, u, 0.0)
        up_ref[here, here] = up

        def trail(k, c):
            there = pl.ds(pl.multiple_of(k * OB, OB), OB)
            prev = jnp.where((lane >= off) & (lane < off + OB), 0.0, m[there, :])
            m[there, :] = prev - dot(m[here, there], u, 0, 0)
            return c

        lax.fori_loop(b + 1, nb, trail, 0)
        return carry

    lax.fori_loop(0, nb, step, 0)
    row = lax.broadcasted_iota(jnp.int32, (size, size), 0)
    col = lax.broadcasted_iota(jnp.int32, (size, size), 1)
    inv_ref[...] = jnp.where(col <= row, m[...], 0.0)


def strips(size, move):
    for p in range(8):
        wide = OB * (p // 4 + 1)
        rest = size - wide
        top, bottom = NB * p, size - NB * (p + 1)
        move(p, 0, NB, slice(0, wide), top, slice(0, wide))
        move(p, 0, NB, slice(wide, size), bottom, slice(0, rest))
        for q in range(4):
            here = slice(OB * q, OB * (q + 1))
            move(p, NB, 8, here, bottom + 8 * q, slice(rest, rest + OB))


def pack(inv, packed):
    def move(p, row, rows, lanes, to_row, to_lanes):
        packed[p, row : row + rows, lanes] = inv[to_row : to_row + rows, to_lanes]

    strips(inv.shape[0], move)


def halves(v):
    high = v.astype(jnp.bfloat16)
    return high, (v - high.astype(jnp.float32)).astype(jnp.bfloat16)


def dot3(a, b, ca, cb):
    total = None
    for p, q in ((a[1], b[0]), (a[0], b[1]), (a[0], b[0])):
        part = lax.dot_general(
            p, q, (((ca,), (cb,)), ((), ())), preferred_element_type=jnp.float32
        )
        total = part if total is None else total + part
    return total


def slot_of(place, p):
    v = lax.bitwise_xor(place[3], p)
    low, high = lax.bitwise_and(v, 1), lax.shift_right_logical(v, 2)
    return 4 * low + lax.bitwise_and(v, 2) + high


def unpack(packed, inv, slots):
    def move(p, row, rows, lanes, to_row, to_lanes):
        inv[to_row : to_row + rows, to_lanes] = packed[slots[p], row : row + rows, lanes]

    inv[...] = jnp.zeros(inv.shape, jnp.float32)
    strips(inv.shape[0], move)


def take_inverse(place, own, one, zero, inv):
    slots = [slot_of(place, p) for p in range(8)]
    owner = place[2] == 1
    on_one = lax.rem(place[1], 2) == 1

    @pl.when(owner)
    def _():
        unpack(own, inv, list(range(8)))

    @pl.when(on_one)
    def _():
        unpack(one, inv, slots)

    @pl.when(jnp.logical_not(owner | on_one))
    def _():
        unpack(zero, inv, slots)


def middle_kernel(
    place, line, swap, own0, one0, zero0, zero_cross, one_cross, x0, link, rest, inv, w1
):
    c = place[0]
    even = lax.rem(place[1], 2) == 0
    size = inv.shape[0]
    part = size // 8
    take_inverse(place, own0, one0, zero0, inv)

    def keep_cross(ref):
        for p in range(8):
            rest[part * p : part * (p + 1)] = ref[slot_of(place, p)]

    @pl.when(even)
    def _():
        keep_cross(zero_cross)

    @pl.when(jnp.logical_not(even))
    def _():
        keep_cross(one_cross)

    def keep(a, b):
        x0[...] = a[...]
        w1[...] = b[...]

    @pl.when(even)
    def _():
        keep(line, swap)

    @pl.when(jnp.logical_not(even))
    def _():
        keep(swap, line)

    il = lax.broadcasted_iota(jnp.int32, (size, size), 1)
    isb = lax.broadcasted_iota(jnp.int32, (size, size), 0)
    eye = jnp.where(il == isb, jnp.float32(1.0), jnp.float32(0.0))
    lower = halves(inv[...])
    cross = halves(rest[...])
    q0 = dot3(lower, halves(x0[...]), 1, 0)
    q0 = jnp.where(c == 0, -eye, jnp.where(c == 1, 0.0, q0))
    x = dot3(lower, halves(q0), 0, 0)
    x0[...] = x
    link[...] = dot3(lower, halves(dot3(lower, cross, 1, 0)), 0, 0)
    rest[...] = w1[...] - dot3(cross, halves(x), 0, 0)


def tail_kernel(place, own1, one1, zero1, x0, link, rest, yh, yl, inv):
    c = place[0]
    size = inv.shape[0]
    take_inverse(place, own1, one1, zero1, inv)
    il = lax.broadcasted_iota(jnp.int32, (size, size), 1)
    isb = lax.broadcasted_iota(jnp.int32, (size, size), 0)
    eye = jnp.where(il == isb, jnp.float32(1.0), jnp.float32(0.0))
    lower = halves(inv[...])
    q1 = dot3(lower, halves(rest[...]), 1, 0)
    q1 = jnp.where(c == 0, 0.0, jnp.where(c == 1, -eye, q1))
    y1 = halves(-dot3(lower, halves(q1), 0, 0))
    y0 = halves(-x0[...] - dot3(halves(link[...]), y1, 1, 0))
    half = size // 2
    for k, y in enumerate((yh, yl)):
        y[0] = y0[k]
        y[1, half:] = y1[k][:half]
        y[1, :half] = y1[k][half:]


def multipliers(kernel, outs, dtype, scratch, place, *ins):
    vm = pl.BlockSpec(memory_space=pltpu.VMEM)
    return pl.pallas_call(
        kernel,
        out_shape=tuple(jax.ShapeDtypeStruct(o, dtype) for o in outs),
        in_specs=[pl.BlockSpec(memory_space=pltpu.SMEM)] + [vm] * len(ins),
        out_specs=(vm,) * len(outs),
        scratch_shapes=[pltpu.VMEM(o, jnp.float32) for o in scratch],
        compiler_params=pltpu.CompilerParams(vmem_limit_bytes=26 << 20),
        name=kernel.__name__,
    )(place, *ins)


def first_kernel(flag, f00, inv, packed, up, tick, m):
    tick[...] = jnp.zeros(tick.shape, jnp.float32)

    @pl.when(flag[0] == 1)
    def _():
        m[...] = f00[...]
        chol_body(inv, up, m)
        pack(inv, packed)


def second_kernel(flag, inv0, f10, f11, inv, packed, up, tick, m):
    tick[...] = jnp.zeros(tick.shape, jnp.float32)

    @pl.when(flag[0] == 1)
    def _():
        q = dot(inv0[...], f10[...], 1, 1)
        m[...] = f11[...] - dot(q, q, 0, 0)
        chol_body(inv, up, m)
        pack(inv, packed)


def factor(kernel, flag, *ins):
    size = ins[0].shape[0]
    out = jax.ShapeDtypeStruct((size, size), jnp.float32)
    packed = jax.ShapeDtypeStruct((8, NB + 8, size), jnp.float32)
    vm = pl.BlockSpec(memory_space=pltpu.VMEM)
    return pl.pallas_call(
        kernel,
        out_shape=(out, packed, out, jax.ShapeDtypeStruct((8, OB), jnp.float32)),
        in_specs=[pl.BlockSpec(memory_space=pltpu.SMEM)] + [vm] * len(ins),
        out_specs=(vm, vm, vm, vm),
        scratch_shapes=[pltpu.VMEM((size, size), jnp.float32)],
        compiler_params=pltpu.CompilerParams(vmem_limit_bytes=24 << 20),
        name=kernel.__name__,
    )(flag, *ins)


def last_kernel(place, g, yh, yl, f, own_diag, out):
    a = pl.program_id(0)
    h = pl.program_id(1)
    c = place[0]
    ident = a * N_ROW + place[1]
    size = yh.shape[1]
    rows = out.shape[2]

    def bf(p, q):
        return jnp.dot(p, q, preferred_element_type=jnp.float32)

    row = lax.broadcasted_iota(jnp.int32, (rows, size), 0) + h * rows
    col = lax.broadcasted_iota(jnp.int32, (rows, size), 1)

    @pl.when((ident > jnp.minimum(c, 1)) | ((ident == 1) & (c == 1)))
    def _():
        total = jnp.where(c >= 2, f[0, 0], 0.0)
        for k in range(2):
            high, low = halves(g[:, k].reshape(size, rows).T)
            total = total + (bf(low, yh[k]) + bf(high, yl[k]) + bf(high, yh[k]))
        out[0, 0] = jnp.where((ident == 1) & (c == 1) & (col > row), 0.0, total)

    @pl.when((ident <= jnp.minimum(c, 1)) & ((ident != c) | (c > 1)))
    def _():
        out[0, 0] = jnp.zeros((rows, size), jnp.float32)

    @pl.when((ident == 0) & (c == 0))
    def _():
        out[0, 0] = own_diag[:, pl.ds(pl.multiple_of(h * rows, rows), rows)].T


def last(place, gathered, high, low, matrix, own_diag):
    count, _, size, _ = matrix.shape
    part = 2
    rows = size // part
    tile = pl.BlockSpec((1, 1, rows, size), lambda a, h: (a, 0, h, 0))
    return pl.pallas_call(
        last_kernel,
        grid=(count, part),
        out_shape=jax.ShapeDtypeStruct(matrix.shape, jnp.float32),
        in_specs=[
            pl.BlockSpec(memory_space=pltpu.SMEM),
            pl.BlockSpec((8, 2, size // 8, rows), lambda a, h: (a, 0, 0, h)),
            pl.BlockSpec((2, size, size), lambda a, h: (0, 0, 0)),
            pl.BlockSpec((2, size, size), lambda a, h: (0, 0, 0)),
            tile,
            pl.BlockSpec((size, size), lambda a, h: (0, 0)),
        ],
        out_specs=tile,
        compiler_params=pltpu.CompilerParams(vmem_limit_bytes=50 << 20),
        name="last",
    )(place, gathered, high, low, matrix, own_diag)


def send(v, pairs):
    return lax.ppermute(v, AXES, pairs)


def later(v, first):
    return v + jnp.minimum(jnp.abs(first[(0,) * first.ndim]), 0.0)


def broadcast(pieces, me, core, x0, skip=(), ahead=None, start=None):
    cols, ys, xs = range(N_COL), range(4), range(4)
    steps = []

    def wait(v):
        return v if ahead is None else later(v, ahead[len(steps)])

    held = jnp.where(me == at(0, core, 0, x0), pieces, 0.0)
    if start is not None:
        held = later(held, start)
    for half in (4, 2, 1):
        pairs = [(at(0, core, k, x0), at(0, core, k + half, x0)) for k in range(0, N_COL, 2 * half)]
        held = wait(held)
        held = held[:half] + send(held[half:], pairs)
        steps.append(held)
    x1, x2, x3 = x0 ^ 1, x0 ^ 2, x0 ^ 3
    for pairs in (
        [(at(0, core, k, x0), at(2, core, k, x0)) for k in cols],
        [(at(y, core, k, x0), at(y + 1, core, k, x0)) for k in cols for y in (0, 2)],
        [(at(y, core, k, x0), at(y, core, k, x2)) for k in cols for y in ys],
        [
            (at(y, core, k, a), at(y, core, k, b))
            for k in cols
            for y in ys
            for a, b in ((x0, x1), (x2, x3))
        ],
    ):
        held = wait(held)
        held = held + send(held, pairs)
        steps.append(held)
    for bit in (4, 2, 1):
        pairs = [(at(y, core, k, x), at(y, core, k ^ bit, x)) for k in cols for y in ys for x in xs]
        held = wait(held)
        held = jnp.concatenate([held, send(held, pairs)])
        steps.append(held)
    pairs = [(at(y, core, k, x), at(y, 1 - core, k, x)) for k in cols for y in ys for x in xs]
    held = wait(held)
    other = send(held, [p for p in pairs if p[1] not in skip])
    steps.append(other)
    return (held, other), steps


def body(matrix):
    mine = matrix[0, 0]
    size = mine.shape[0]
    r = lax.axis_index("row")
    z = lax.axis_index("col")
    c = lax.axis_index(("col", "depth"))
    me = lax.axis_index(AXES)
    owner = me == OWNER
    place = jnp.stack([c, r, owner.astype(jnp.int32), z]).astype(jnp.int32)
    flag = owner.astype(jnp.int32).reshape(1)

    inv0, packed0, up0, tick = factor(first_kernel, flag, mine)
    f10 = send(mine, [(ROOT, OWNER)])
    f11 = send(mine, [(dev(1, 1), OWNER)])

    step = size // 8
    after = later(mine, tick)
    got = []
    for k in range(8):
        pairs = [(dev(0, j), dev(j % 8, 8 * (j // 8) + k)) for j in range(1, N_BC)]
        pairs += [(dev(1, j), dev(j % 8, 8 * (j // 8) + (k + 4) % 8)) for j in range(1, N_BC)]
        got.append(send(after[k * step : (k + 1) * step], pairs))
    slot = c % 8
    first = sum(jnp.where(slot == k, got[k], 0.0) for k in range(8))
    second = sum(jnp.where(slot == (k + 4) % 8, got[k], 0.0) for k in range(8))
    shares, mine, f10, f11, packed0 = lax.optimization_barrier(
        (jnp.stack([first, second]), mine, f10, f11, packed0)
    )
    gathered = lax.all_gather(shares, ("col", "depth"))

    root0 = send(packed0, [(OWNER, ROOT)])
    _, packed1, _, tick = factor(second_kernel, flag, inv0, f10, f11)
    root1 = send(packed1, [(OWNER, ROOT)])
    cross, cross_steps = broadcast(later(mine, tick).reshape(8, step, size), me, 0, 1)
    first, steps = broadcast(root0, me, 1, 0, (OWNER,))
    spread = steps[6]
    second, _ = broadcast(root1, me, 1, 0, (OWNER,), steps, spread)

    cs = range(2, N_BC)
    line = later(jnp.where(r < 2, mine, 0.0), cross_steps[4])
    line = line + send(line, [(dev(a, j), dev(a + 2, j)) for j in cs for a in (0, 1)])
    line = later(line, spread)
    hops = [(0, 6), (1, 7), (2, 4), (3, 5)]
    line = line + send(line, [(dev(a, j), dev(b, j)) for j in cs for a, b in hops])
    swap = send(line, [(dev(a, j), dev(a ^ 1, j)) for j in cs for a in range(8)])

    block = (size, size)
    x0, link, rest = multipliers(
        middle_kernel, [block] * 3, jnp.float32, [block] * 2, place, line, swap, packed0, *first, *cross
    )
    high, low = multipliers(
        tail_kernel, [(2,) + block] * 2, jnp.bfloat16, [block], place, packed1, *second, x0, link, rest
    )
    return last(place, gathered, high, low, matrix, up0)


def solution(mesh):
    placed = P(None, "row", None, ("col", "depth"))
    return jax.shard_map(body, mesh=mesh, in_specs=(placed,), out_specs=placed, check_vma=False)
```

```python
import jax
import jax.numpy as jnp
from jax import lax
from jax.experimental import pallas as pl
from jax.experimental.pallas import tpu as pltpu
from jax.sharding import PartitionSpec as P

HI = lax.Precision.HIGHEST
NB = 32
OB = 128
AXES = ("row", "col", "depth")
N_ROW = 8
N_COL = 8
N_DEPTH = 4
N_BC = N_COL * N_DEPTH


def dev(r, c):
    return r * N_BC + c


def at(y, core, z, x):
    return dev(2 * y + core, z * N_DEPTH + x)


OWNER = dev(0, 0)
ROOT = dev(1, 0)


def dot(a, b, ca, cb, precision=HI):
    return lax.dot_general(
        a, b, (((ca,), (cb,)), ((), ())), precision=precision, preferred_element_type=jnp.float32
    )


def eliminate(rows, lane0):
    lanes = lax.broadcasted_iota(jnp.int32, (NB, OB), 1)
    subl = lax.broadcasted_iota(jnp.int32, (NB, OB), 0)
    ident = jnp.where(lanes == subl + lane0, jnp.float32(1.0), jnp.float32(0.0))
    groups = NB // 8

    def split(v):
        return [v[8 * g : 8 * g + 8] for g in range(groups)]

    cols = [
        split(jnp.broadcast_to(rows[:, lane0 + j : lane0 + j + 1], (NB, OB))) for j in range(NB)
    ]
    a = split(rows)
    x = split(ident)
    sub8 = lax.broadcasted_iota(jnp.int32, (8, OB), 0)
    for j in range(NB):
        gj, rj = j // 8, j % 8
        inv = lax.rsqrt(jnp.broadcast_to(cols[j][gj][rj : rj + 1], (8, OB)))
        lcol = [cols[j][g] * inv if g >= gj else None for g in range(groups)]
        ua = jnp.broadcast_to(a[gj][rj : rj + 1], (8, OB)) * inv
        ux = jnp.broadcast_to(x[gj][rj : rj + 1], (8, OB)) * inv
        mine = sub8 == rj
        if rj < 7:
            lself = jnp.where(sub8 > rj, lcol[gj], 0.0)
            a[gj] = jnp.where(mine, ua, a[gj] - lself * ua)
            x[gj] = jnp.where(mine, ux, x[gj] - lself * ux)
        else:
            a[gj] = jnp.where(mine, ua, a[gj])
            x[gj] = jnp.where(mine, ux, x[gj])
        for g in range(gj + 1, groups):
            a[g] = a[g] - lcol[g] * ua
            x[g] = x[g] - lcol[g] * ux
        for k in range(j + 1, NB):
            gk, rk = k // 8, k % 8
            s = jnp.broadcast_to(lcol[gk][rk : rk + 1], (8, OB))
            for g in range(gk, groups):
                cols[k][g] = cols[k][g] - lcol[g] * s
    return jnp.concatenate(a, axis=0), jnp.concatenate(x, axis=0)


def diag_block(w):
    n = OB // NB
    lanes = lax.broadcasted_iota(jnp.int32, (NB, OB), 1)
    subl = lax.broadcasted_iota(jnp.int32, (NB, OB), 0)
    wl = lax.broadcasted_iota(jnp.int32, (OB, OB), 1)
    ups = []
    done = []
    for i in range(n):
        lo = NB * i
        ua, ux = eliminate(w[lo : lo + NB], lo)
        inblk = (lanes >= lo) & (lanes < lo + NB)
        ups.append(jnp.where(lanes >= subl + lo, ua, 0.0))
        u = jnp.where(inblk, jnp.where(lanes <= subl + lo, ux, 0.0), ua)
        if i + 1 < n:
            um = jnp.where(lanes >= lo + NB, u, 0.0)
            w = jnp.where((wl >= lo) & (wl < lo + NB), 0.0, w) - dot(um, u, 0, 0)
        done.append(u)
        w = jnp.concatenate(done + [w[NB * (i + 1) :]] if i + 1 < n else done, axis=0)
    return w, jnp.concatenate(ups, axis=0)


def chol_body(inv_ref, up_ref, m):
    size = m.shape[0]
    nb = size // OB
    up_ref[...] = jnp.zeros((size, size), jnp.float32)
    il = lax.broadcasted_iota(jnp.int32, (OB, OB), 1)
    isb = lax.broadcasted_iota(jnp.int32, (OB, OB), 0)
    lane = lax.broadcasted_iota(jnp.int32, (OB, size), 1)

    def step(b, carry):
        off = pl.multiple_of(b * OB, OB)
        here = pl.ds(off, OB)
        inv, up = diag_block(m[here, here])
        inv = jnp.where(il <= isb, inv, 0.0)
        m[here, here] = jnp.where(il == isb, jnp.float32(1.0), jnp.float32(0.0))
        u = dot(inv, m[here, :], 1, 0)
        m[here, :] = u
        up_ref[here, :] = jnp.where(lane >= off + OB, u, 0.0)
        up_ref[here, here] = up

        def trail(k, c):
            there = pl.ds(pl.multiple_of(k * OB, OB), OB)
            prev = jnp.where((lane >= off) & (lane < off + OB), 0.0, m[there, :])
            m[there, :] = prev - dot(m[here, there], u, 0, 0)
            return c

        lax.fori_loop(b + 1, nb, trail, 0)
        return carry

    lax.fori_loop(0, nb, step, 0)
    row = lax.broadcasted_iota(jnp.int32, (size, size), 0)
    col = lax.broadcasted_iota(jnp.int32, (size, size), 1)
    inv_ref[...] = jnp.where(col <= row, m[...], 0.0)


def strips(size, move):
    for p in range(8):
        wide = OB * (p // 4 + 1)
        rest = size - wide
        top, bottom = NB * p, size - NB * (p + 1)
        move(p, 0, NB, slice(0, wide), top, slice(0, wide))
        move(p, 0, NB, slice(wide, size), bottom, slice(0, rest))
        for q in range(4):
            here = slice(OB * q, OB * (q + 1))
            move(p, NB, 8, here, bottom + 8 * q, slice(rest, rest + OB))


def pack(inv, packed):
    def move(p, row, rows, lanes, to_row, to_lanes):
        packed[p, row : row + rows, lanes] = inv[to_row : to_row + rows, to_lanes]

    strips(inv.shape[0], move)


def halves(v):
    high = v.astype(jnp.bfloat16)
    return high, (v - high.astype(jnp.float32)).astype(jnp.bfloat16)


def dot3(a, b, ca, cb):
    total = None
    for p, q in ((a[1], b[0]), (a[0], b[1]), (a[0], b[0])):
        part = lax.dot_general(
            p, q, (((ca,), (cb,)), ((), ())), preferred_element_type=jnp.float32
        )
        total = part if total is None else total + part
    return total


def slot_of(place, p):
    v = lax.bitwise_xor(place[3], p)
    low, high = lax.bitwise_and(v, 1), lax.shift_right_logical(v, 2)
    return 4 * low + lax.bitwise_and(v, 2) + high


def take_inverse(place, own, one, zero, inv):
    slots = [slot_of(place, p) for p in range(8)]
    owner = place[2] == 1
    on_one = lax.rem(place[1], 2) == 1

    def move(p, row, rows, lanes, to_row, to_lanes):
        here = slice(row, row + rows)
        got = jnp.where(on_one, one[slots[p], here, lanes], zero[slots[p], here, lanes])
        inv[to_row : to_row + rows, to_lanes] = jnp.where(owner, own[p, here, lanes], got)

    inv[...] = jnp.zeros(inv.shape, jnp.float32)
    strips(inv.shape[0], move)


def middle_kernel(
    place, line, swap, own0, one0, zero0, zero_cross, one_cross, x0, link, rest, inv, w1
):
    c = place[0]
    even = lax.rem(place[1], 2) == 0
    size = inv.shape[0]
    part = size // 8
    take_inverse(place, own0, one0, zero0, inv)

    for p in range(8):
        slot = slot_of(place, p)
        rest[part * p : part * (p + 1)] = jnp.where(even, zero_cross[slot], one_cross[slot])
    x0[...] = jnp.where(even, line[...], swap[...])
    w1[...] = jnp.where(even, swap[...], line[...])

    il = lax.broadcasted_iota(jnp.int32, (size, size), 1)
    isb = lax.broadcasted_iota(jnp.int32, (size, size), 0)
    eye = jnp.where(il == isb, jnp.float32(1.0), jnp.float32(0.0))
    lower = halves(inv[...])
    cross = halves(rest[...])
    q0 = dot3(lower, halves(x0[...]), 1, 0)
    q0 = jnp.where(c == 0, -eye, jnp.where(c == 1, 0.0, q0))
    x = dot3(lower, halves(q0), 0, 0)
    x0[...] = x
    link[...] = dot3(lower, halves(dot3(lower, cross, 1, 0)), 0, 0)
    rest[...] = w1[...] - dot3(cross, halves(x), 0, 0)


def tail_kernel(place, own1, one1, zero1, x0, link, rest, yh, yl, inv):
    c = place[0]
    size = inv.shape[0]
    take_inverse(place, own1, one1, zero1, inv)
    il = lax.broadcasted_iota(jnp.int32, (size, size), 1)
    isb = lax.broadcasted_iota(jnp.int32, (size, size), 0)
    eye = jnp.where(il == isb, jnp.float32(1.0), jnp.float32(0.0))
    lower = halves(inv[...])
    q1 = dot3(lower, halves(rest[...]), 1, 0)
    q1 = jnp.where(c == 0, 0.0, jnp.where(c == 1, -eye, q1))
    y1 = halves(-dot3(lower, halves(q1), 0, 0))
    y0 = halves(-x0[...] - dot3(halves(link[...]), y1, 1, 0))
    half = size // 2
    for k, y in enumerate((yh, yl)):
        y[0] = y0[k]
        y[1, half:] = y1[k][:half]
        y[1, :half] = y1[k][half:]


def multipliers(kernel, outs, dtype, scratch, place, *ins):
    vm = pl.BlockSpec(memory_space=pltpu.VMEM)
    return pl.pallas_call(
        kernel,
        out_shape=tuple(jax.ShapeDtypeStruct(o, dtype) for o in outs),
        in_specs=[pl.BlockSpec(memory_space=pltpu.SMEM)] + [vm] * len(ins),
        out_specs=(vm,) * len(outs),
        scratch_shapes=[pltpu.VMEM(o, jnp.float32) for o in scratch],
        compiler_params=pltpu.CompilerParams(vmem_limit_bytes=26 << 20),
        name=kernel.__name__,
    )(place, *ins)


def first_kernel(flag, f00, inv, packed, up, tick, m):
    tick[...] = jnp.zeros(tick.shape, jnp.float32)

    @pl.when(flag[0] == 1)
    def _():
        m[...] = f00[...]
        chol_body(inv, up, m)
        pack(inv, packed)


def second_kernel(flag, inv0, f10, f11, inv, packed, up, tick, m):
    tick[...] = jnp.zeros(tick.shape, jnp.float32)

    @pl.when(flag[0] == 1)
    def _():
        count = m.shape[0] // OB

        def solve(b, carry):
            here = pl.ds(pl.multiple_of(b * OB, OB), OB)
            up[here, :] = dot(inv0[here, :], f10[...], 1, 1)
            return carry

        def update(b, carry):
            here = pl.ds(pl.multiple_of(b * OB, OB), OB)
            m[here, :] = f11[here, :] - dot(up[:, here], up[...], 0, 0)
            return carry

        lax.fori_loop(0, count, solve, 0)
        lax.fori_loop(0, count, update, 0)
        chol_body(inv, up, m)
        pack(inv, packed)


def factor(kernel, flag, *ins):
    size = ins[0].shape[0]
    out = jax.ShapeDtypeStruct((size, size), jnp.float32)
    packed = jax.ShapeDtypeStruct((8, NB + 8, size), jnp.float32)
    vm = pl.BlockSpec(memory_space=pltpu.VMEM)
    return pl.pallas_call(
        kernel,
        out_shape=(out, packed, out, jax.ShapeDtypeStruct((8, OB), jnp.float32)),
        in_specs=[pl.BlockSpec(memory_space=pltpu.SMEM)] + [vm] * len(ins),
        out_specs=(vm, vm, vm, vm),
        scratch_shapes=[pltpu.VMEM((size, size), jnp.float32)],
        compiler_params=pltpu.CompilerParams(vmem_limit_bytes=24 << 20),
        name=kernel.__name__,
    )(flag, *ins)


def last_kernel(place, g, yh, yl, f, own_diag, out):
    a = pl.program_id(0)
    h = pl.program_id(1)
    c = place[0]
    ident = a * N_ROW + place[1]
    size = yh.shape[1]
    rows = out.shape[2]

    def bf(p, q):
        return jnp.dot(p, q, preferred_element_type=jnp.float32)

    row = lax.broadcasted_iota(jnp.int32, (rows, size), 0) + h * rows
    col = lax.broadcasted_iota(jnp.int32, (rows, size), 1)

    @pl.when((ident > jnp.minimum(c, 1)) | ((ident == 1) & (c == 1)))
    def _():
        total = jnp.where(c >= 2, f[0, 0], 0.0)
        for k in range(2):
            high, low = halves(g[:, k].reshape(size, rows).T)
            total = total + (bf(low, yh[k]) + bf(high, yl[k]) + bf(high, yh[k]))
        out[0, 0] = jnp.where((ident == 1) & (c == 1) & (col > row), 0.0, total)

    @pl.when((ident <= jnp.minimum(c, 1)) & ((ident != c) | (c > 1)))
    def _():
        out[0, 0] = jnp.zeros((rows, size), jnp.float32)

    @pl.when((ident == 0) & (c == 0))
    def _():
        out[0, 0] = own_diag[:, pl.ds(pl.multiple_of(h * rows, rows), rows)].T


def last(place, gathered, high, low, matrix, own_diag):
    count, _, size, _ = matrix.shape
    part = 2
    rows = size // part
    tile = pl.BlockSpec((1, 1, rows, size), lambda a, h: (a, 0, h, 0))
    return pl.pallas_call(
        last_kernel,
        grid=(count, part),
        out_shape=jax.ShapeDtypeStruct(matrix.shape, jnp.float32),
        in_specs=[
            pl.BlockSpec(memory_space=pltpu.SMEM),
            pl.BlockSpec((8, 2, size // 8, rows), lambda a, h: (a, 0, 0, h)),
            pl.BlockSpec((2, size, size), lambda a, h: (0, 0, 0)),
            pl.BlockSpec((2, size, size), lambda a, h: (0, 0, 0)),
            tile,
            pl.BlockSpec((size, size), lambda a, h: (0, 0)),
        ],
        out_specs=tile,
        compiler_params=pltpu.CompilerParams(vmem_limit_bytes=50 << 20),
        name="last",
    )(place, gathered, high, low, matrix, own_diag)


def send(v, pairs):
    return lax.ppermute(v, AXES, pairs)


def later(v, first):
    return v + jnp.minimum(jnp.abs(first[(-1,) * first.ndim]), 0.0)


def broadcast(pieces, me, core, x0, skip=(), ahead=None, start=None):
    cols, ys, xs = range(N_COL), range(4), range(4)
    steps = []

    def wait(v):
        return v if ahead is None else later(v, ahead[len(steps)])

    held = jnp.where(me == at(0, core, 0, x0), pieces, 0.0)
    if start is not None:
        held = later(held, start)
    for half in (4, 2, 1):
        pairs = [(at(0, core, k, x0), at(0, core, k + half, x0)) for k in range(0, N_COL, 2 * half)]
        held = wait(held)
        held = held[:half] + send(held[half:], pairs)
        steps.append(held)
    x1, x2, x3 = x0 ^ 1, x0 ^ 2, x0 ^ 3
    for pairs in (
        [(at(0, core, k, x0), at(2, core, k, x0)) for k in cols],
        [(at(y, core, k, x0), at(y + 1, core, k, x0)) for k in cols for y in (0, 2)],
        [(at(y, core, k, x0), at(y, core, k, x2)) for k in cols for y in ys],
        [
            (at(y, core, k, a), at(y, core, k, b))
            for k in cols
            for y in ys
            for a, b in ((x0, x1), (x2, x3))
        ],
    ):
        held = wait(held)
        held = held + send(held, pairs)
        steps.append(held)
    for bit in (4, 2, 1):
        pairs = [(at(y, core, k, x), at(y, core, k ^ bit, x)) for k in cols for y in ys for x in xs]
        held = wait(held)
        held = jnp.concatenate([held, send(held, pairs)])
        steps.append(held)
    pairs = [(at(y, core, k, x), at(y, 1 - core, k, x)) for k in cols for y in ys for x in xs]
    held = wait(held)
    other = send(held, [p for p in pairs if p[1] not in skip])
    steps.append(other)
    return (held, other), steps


def body(matrix):
    mine = matrix[0, 0]
    size = mine.shape[0]
    r = lax.axis_index("row")
    z = lax.axis_index("col")
    c = lax.axis_index(("col", "depth"))
    me = lax.axis_index(AXES)
    owner = me == OWNER
    place = jnp.stack([c, r, owner.astype(jnp.int32), z]).astype(jnp.int32)
    flag = owner.astype(jnp.int32).reshape(1)

    inv0, packed0, up0, tick = factor(first_kernel, flag, mine)
    f10 = send(mine, [(ROOT, OWNER)])
    f11 = send(mine, [(dev(1, 1), OWNER)])

    step = size // 8
    after = later(mine, tick)
    got = []
    for k in range(8):
        pairs = [(dev(0, j), dev(j % 8, 8 * (j // 8) + k)) for j in range(1, N_BC)]
        pairs += [(dev(1, j), dev(j % 8, 8 * (j // 8) + (k + 4) % 8)) for j in range(1, N_BC)]
        got.append(send(after[k * step : (k + 1) * step], pairs))
    slot = c % 8
    first = sum(jnp.where(slot == k, got[k], 0.0) for k in range(8))
    second = sum(jnp.where(slot == (k + 4) % 8, got[k], 0.0) for k in range(8))
    shares, mine, f10, f11, packed0 = lax.optimization_barrier(
        (jnp.stack([first, second]), mine, f10, f11, packed0)
    )
    gathered = lax.all_gather(shares, ("col", "depth"))

    root0 = send(packed0, [(OWNER, ROOT)])
    _, packed1, _, tick = factor(second_kernel, flag, inv0, f10, f11)
    root1 = send(packed1, [(OWNER, ROOT)])
    cross, cross_steps = broadcast(later(mine, tick).reshape(8, step, size), me, 0, 1)
    first, steps = broadcast(root0, me, 1, 0, (OWNER,))
    spread = steps[6]
    second, _ = broadcast(root1, me, 1, 0, (OWNER,), steps, steps[9])

    cs = range(2, N_BC)
    line = later(jnp.where(r < 2, mine, 0.0), cross_steps[4])
    line = line + send(line, [(dev(a, j), dev(a + 2, j)) for j in cs for a in (0, 1)])
    line = later(line, spread)
    hops = [(0, 6), (1, 7), (2, 4), (3, 5)]
    line = line + send(line, [(dev(a, j), dev(b, j)) for j in cs for a, b in hops])
    swap = send(line, [(dev(a, j), dev(a ^ 1, j)) for j in cs for a in range(8)])

    block = (size, size)
    x0, link, rest = multipliers(
        middle_kernel, [block] * 3, jnp.float32, [block] * 2, place, line, swap, packed0, *first, *cross
    )
    high, low = multipliers(
        tail_kernel, [(2,) + block] * 2, jnp.bfloat16, [block], place, packed1, *second, x0, link, rest
    )
    return last(place, gathered, high, low, matrix, up0)


def solution(mesh):
    placed = P(None, "row", None, ("col", "depth"))
    return jax.shard_map(body, mesh=mesh, in_specs=(placed,), out_specs=placed, check_vma=False)
```

```python
import jax
import jax.numpy as jnp
from jax import lax
from jax.experimental import pallas as pl
from jax.experimental.pallas import tpu as pltpu
from jax.sharding import PartitionSpec as P

HI = lax.Precision.HIGHEST
NB = 32
OB = 128
AXES = ("row", "col", "depth")
N_ROW = 8
N_COL = 8
N_DEPTH = 4
N_BC = N_COL * N_DEPTH


def dev(r, c):
    return r * N_BC + c


def at(y, core, z, x):
    return dev(2 * y + core, z * N_DEPTH + x)


OWNER = dev(0, 0)
ROOT = dev(1, 0)


def dot(a, b, ca, cb, precision=HI):
    return lax.dot_general(
        a, b, (((ca,), (cb,)), ((), ())), precision=precision, preferred_element_type=jnp.float32
    )


def eliminate(rows, lane0):
    lanes = lax.broadcasted_iota(jnp.int32, (NB, OB), 1)
    subl = lax.broadcasted_iota(jnp.int32, (NB, OB), 0)
    ident = jnp.where(lanes == subl + lane0, jnp.float32(1.0), jnp.float32(0.0))
    groups = NB // 8

    def split(v):
        return [v[8 * g : 8 * g + 8] for g in range(groups)]

    cols = [
        split(jnp.broadcast_to(rows[:, lane0 + j : lane0 + j + 1], (NB, OB))) for j in range(NB)
    ]
    a = split(rows)
    x = split(ident)
    sub8 = lax.broadcasted_iota(jnp.int32, (8, OB), 0)
    for j in range(NB):
        gj, rj = j // 8, j % 8
        inv = lax.rsqrt(jnp.broadcast_to(cols[j][gj][rj : rj + 1], (8, OB)))
        lcol = [cols[j][g] * inv if g >= gj else None for g in range(groups)]
        ua = jnp.broadcast_to(a[gj][rj : rj + 1], (8, OB)) * inv
        ux = jnp.broadcast_to(x[gj][rj : rj + 1], (8, OB)) * inv
        mine = sub8 == rj
        if rj < 7:
            lself = jnp.where(sub8 > rj, lcol[gj], 0.0)
            a[gj] = jnp.where(mine, ua, a[gj] - lself * ua)
            x[gj] = jnp.where(mine, ux, x[gj] - lself * ux)
        else:
            a[gj] = jnp.where(mine, ua, a[gj])
            x[gj] = jnp.where(mine, ux, x[gj])
        for g in range(gj + 1, groups):
            a[g] = a[g] - lcol[g] * ua
            x[g] = x[g] - lcol[g] * ux
        for k in range(j + 1, NB):
            gk, rk = k // 8, k % 8
            s = jnp.broadcast_to(lcol[gk][rk : rk + 1], (8, OB))
            for g in range(gk, groups):
                cols[k][g] = cols[k][g] - lcol[g] * s
    return jnp.concatenate(a, axis=0), jnp.concatenate(x, axis=0)


def diag_block(w):
    n = OB // NB
    lanes = lax.broadcasted_iota(jnp.int32, (NB, OB), 1)
    subl = lax.broadcasted_iota(jnp.int32, (NB, OB), 0)
    wl = lax.broadcasted_iota(jnp.int32, (OB, OB), 1)
    ups = []
    done = []
    for i in range(n):
        lo = NB * i
        ua, ux = eliminate(w[lo : lo + NB], lo)
        inblk = (lanes >= lo) & (lanes < lo + NB)
        ups.append(jnp.where(lanes >= subl + lo, ua, 0.0))
        u = jnp.where(inblk, jnp.where(lanes <= subl + lo, ux, 0.0), ua)
        if i + 1 < n:
            um = jnp.where(lanes >= lo + NB, u, 0.0)
            w = jnp.where((wl >= lo) & (wl < lo + NB), 0.0, w) - dot(um, u, 0, 0)
        done.append(u)
        w = jnp.concatenate(done + [w[NB * (i + 1) :]] if i + 1 < n else done, axis=0)
    return w, jnp.concatenate(ups, axis=0)


def chol_body(inv_ref, up_ref, m):
    size = m.shape[0]
    nb = size // OB
    up_ref[...] = jnp.zeros((size, size), jnp.float32)
    il = lax.broadcasted_iota(jnp.int32, (OB, OB), 1)
    isb = lax.broadcasted_iota(jnp.int32, (OB, OB), 0)
    lane = lax.broadcasted_iota(jnp.int32, (OB, size), 1)

    def step(b, carry):
        off = pl.multiple_of(b * OB, OB)
        here = pl.ds(off, OB)
        inv, up = diag_block(m[here, here])
        inv = jnp.where(il <= isb, inv, 0.0)
        m[here, here] = jnp.where(il == isb, jnp.float32(1.0), jnp.float32(0.0))
        u = dot(inv, m[here, :], 1, 0)
        m[here, :] = u
        up_ref[here, :] = jnp.where(lane >= off + OB, u, 0.0)
        up_ref[here, here] = up

        def trail(k, c):
            there = pl.ds(pl.multiple_of(k * OB, OB), OB)
            prev = jnp.where((lane >= off) & (lane < off + OB), 0.0, m[there, :])
            m[there, :] = prev - dot(m[here, there], u, 0, 0)
            return c

        lax.fori_loop(b + 1, nb, trail, 0)
        return carry

    lax.fori_loop(0, nb, step, 0)
    row = lax.broadcasted_iota(jnp.int32, (size, size), 0)
    col = lax.broadcasted_iota(jnp.int32, (size, size), 1)
    inv_ref[...] = jnp.where(col <= row, m[...], 0.0)


def strips(size, move):
    for p in range(8):
        wide = OB * (p // 4 + 1)
        rest = size - wide
        top, bottom = NB * p, size - NB * (p + 1)
        move(p, 0, NB, slice(0, wide), top, slice(0, wide))
        move(p, 0, NB, slice(wide, size), bottom, slice(0, rest))
        for q in range(4):
            here = slice(OB * q, OB * (q + 1))
            move(p, NB, 8, here, bottom + 8 * q, slice(rest, rest + OB))


def pack(inv, packed):
    def move(p, row, rows, lanes, to_row, to_lanes):
        packed[p, row : row + rows, lanes] = inv[to_row : to_row + rows, to_lanes]

    strips(inv.shape[0], move)


def halves(v):
    high = v.astype(jnp.bfloat16)
    return high, (v - high.astype(jnp.float32)).astype(jnp.bfloat16)


def dot3(a, b, ca, cb):
    total = None
    for p, q in ((a[1], b[0]), (a[0], b[1]), (a[0], b[0])):
        part = lax.dot_general(
            p, q, (((ca,), (cb,)), ((), ())), preferred_element_type=jnp.float32
        )
        total = part if total is None else total + part
    return total


def slot_of(place, p):
    v = lax.bitwise_xor(place[3], p)
    low, high = lax.bitwise_and(v, 1), lax.shift_right_logical(v, 2)
    return 4 * low + lax.bitwise_and(v, 2) + high


def take_inverse(place, own, one, zero, inv):
    slots = [slot_of(place, p) for p in range(8)]
    owner = place[2] == 1
    on_one = lax.rem(place[1], 2) == 1

    def move(p, row, rows, lanes, to_row, to_lanes):
        here = slice(row, row + rows)
        got = jnp.where(on_one, one[slots[p], here, lanes], zero[slots[p], here, lanes])
        inv[to_row : to_row + rows, to_lanes] = jnp.where(owner, own[p, here, lanes], got)

    inv[...] = jnp.zeros(inv.shape, jnp.float32)
    strips(inv.shape[0], move)


def middle_kernel(
    place, line, swap, own0, one0, zero0, zero_cross, one_cross, x0, link, rest, inv, w1
):
    c = place[0]
    even = lax.rem(place[1], 2) == 0
    size = inv.shape[0]
    part = size // 8
    take_inverse(place, own0, one0, zero0, inv)

    for p in range(8):
        slot = slot_of(place, p)
        rest[part * p : part * (p + 1)] = jnp.where(even, zero_cross[slot], one_cross[slot])
    x0[...] = jnp.where(even, line[...], swap[...])
    w1[...] = jnp.where(even, swap[...], line[...])

    il = lax.broadcasted_iota(jnp.int32, (size, size), 1)
    isb = lax.broadcasted_iota(jnp.int32, (size, size), 0)
    eye = jnp.where(il == isb, jnp.float32(1.0), jnp.float32(0.0))
    lower = halves(inv[...])
    cross = halves(rest[...])
    q0 = dot3(lower, halves(x0[...]), 1, 0)
    q0 = jnp.where(c == 0, -eye, jnp.where(c == 1, 0.0, q0))
    x = dot3(lower, halves(q0), 0, 0)
    x0[...] = x
    link[...] = dot3(lower, halves(dot3(lower, cross, 1, 0)), 0, 0)
    rest[...] = w1[...] - dot3(cross, halves(x), 0, 0)


def tail_kernel(place, own1, one1, zero1, x0, link, rest, yh, yl, inv):
    c = place[0]
    size = inv.shape[0]
    take_inverse(place, own1, one1, zero1, inv)
    il = lax.broadcasted_iota(jnp.int32, (size, size), 1)
    isb = lax.broadcasted_iota(jnp.int32, (size, size), 0)
    eye = jnp.where(il == isb, jnp.float32(1.0), jnp.float32(0.0))
    lower = halves(inv[...])
    q1 = dot3(lower, halves(rest[...]), 1, 0)
    q1 = jnp.where(c == 0, 0.0, jnp.where(c == 1, -eye, q1))
    y1 = halves(-dot3(lower, halves(q1), 0, 0))
    y0 = halves(-x0[...] - dot3(halves(link[...]), y1, 1, 0))
    half = size // 2
    for k, y in enumerate((yh, yl)):
        y[0] = y0[k]
        y[1, half:] = y1[k][:half]
        y[1, :half] = y1[k][half:]


def multipliers(kernel, outs, dtype, scratch, place, *ins):
    vm = pl.BlockSpec(memory_space=pltpu.VMEM)
    return pl.pallas_call(
        kernel,
        out_shape=tuple(jax.ShapeDtypeStruct(o, dtype) for o in outs),
        in_specs=[pl.BlockSpec(memory_space=pltpu.SMEM)] + [vm] * len(ins),
        out_specs=(vm,) * len(outs),
        scratch_shapes=[pltpu.VMEM(o, jnp.float32) for o in scratch],
        compiler_params=pltpu.CompilerParams(vmem_limit_bytes=26 << 20),
        name=kernel.__name__,
    )(place, *ins)


def first_kernel(flag, f00, inv, packed, up, tick, m):
    tick[...] = jnp.zeros(tick.shape, jnp.float32)

    @pl.when(flag[0] == 1)
    def _():
        m[...] = f00[...]
        chol_body(inv, up, m)
        pack(inv, packed)


def second_kernel(flag, inv0, f10, f11, inv, packed, up, tick, m):
    tick[...] = jnp.zeros(tick.shape, jnp.float32)

    @pl.when(flag[0] == 1)
    def _():
        q = dot(inv0[...], f10[...], 1, 1)
        m[...] = f11[...] - dot(q, q, 0, 0)
        chol_body(inv, up, m)
        pack(inv, packed)


def factor(kernel, flag, *ins):
    size = ins[0].shape[0]
    out = jax.ShapeDtypeStruct((size, size), jnp.float32)
    packed = jax.ShapeDtypeStruct((8, NB + 8, size), jnp.float32)
    vm = pl.BlockSpec(memory_space=pltpu.VMEM)
    return pl.pallas_call(
        kernel,
        out_shape=(out, packed, out, jax.ShapeDtypeStruct((8, OB), jnp.float32)),
        in_specs=[pl.BlockSpec(memory_space=pltpu.SMEM)] + [vm] * len(ins),
        out_specs=(vm, vm, vm, vm),
        scratch_shapes=[pltpu.VMEM((size, size), jnp.float32)],
        compiler_params=pltpu.CompilerParams(vmem_limit_bytes=24 << 20),
        name=kernel.__name__,
    )(flag, *ins)


def last_kernel(place, g, yh, yl, f, own_diag, out):
    a = pl.program_id(0)
    h = pl.program_id(1)
    c = place[0]
    ident = a * N_ROW + place[1]
    size = yh.shape[1]
    rows = out.shape[2]

    def bf(p, q):
        return jnp.dot(p, q, preferred_element_type=jnp.float32)

    row = lax.broadcasted_iota(jnp.int32, (rows, size), 0) + h * rows
    col = lax.broadcasted_iota(jnp.int32, (rows, size), 1)

    @pl.when((ident > jnp.minimum(c, 1)) | ((ident == 1) & (c == 1)))
    def _():
        total = jnp.where(c >= 2, f[0, 0], 0.0)
        for k in range(2):
            high, low = halves(g[:, k].reshape(size, rows).T)
            total = total + (bf(low, yh[k]) + bf(high, yl[k]) + bf(high, yh[k]))
        out[0, 0] = jnp.where((ident == 1) & (c == 1) & (col > row), 0.0, total)

    @pl.when((ident <= jnp.minimum(c, 1)) & ((ident != c) | (c > 1)))
    def _():
        out[0, 0] = jnp.zeros((rows, size), jnp.float32)

    @pl.when((ident == 0) & (c == 0))
    def _():
        out[0, 0] = own_diag[:, pl.ds(pl.multiple_of(h * rows, rows), rows)].T


def last(place, gathered, high, low, matrix, own_diag):
    count, _, size, _ = matrix.shape
    part = 2
    rows = size // part
    tile = pl.BlockSpec((1, 1, rows, size), lambda a, h: (a, 0, h, 0))
    return pl.pallas_call(
        last_kernel,
        grid=(count, part),
        out_shape=jax.ShapeDtypeStruct(matrix.shape, jnp.float32),
        in_specs=[
            pl.BlockSpec(memory_space=pltpu.SMEM),
            pl.BlockSpec((8, 2, size // 8, rows), lambda a, h: (a, 0, 0, h)),
            pl.BlockSpec((2, size, size), lambda a, h: (0, 0, 0)),
            pl.BlockSpec((2, size, size), lambda a, h: (0, 0, 0)),
            tile,
            pl.BlockSpec((size, size), lambda a, h: (0, 0)),
        ],
        out_specs=tile,
        compiler_params=pltpu.CompilerParams(vmem_limit_bytes=50 << 20),
        name="last",
    )(place, gathered, high, low, matrix, own_diag)


def send(v, pairs):
    return lax.ppermute(v, AXES, pairs)


def later(v, first):
    return v + jnp.minimum(jnp.abs(first[(0,) * first.ndim]), 0.0)


def broadcast(pieces, me, core, x0, skip=(), ahead=None, start=None):
    cols, ys, xs = range(N_COL), range(4), range(4)
    steps = []

    def wait(v):
        return v if ahead is None else later(v, ahead[len(steps)])

    held = jnp.where(me == at(0, core, 0, x0), pieces, 0.0)
    if start is not None:
        held = later(held, start)
    for half in (4, 2, 1):
        pairs = [(at(0, core, k, x0), at(0, core, k + half, x0)) for k in range(0, N_COL, 2 * half)]
        held = wait(held)
        held = held[:half] + send(held[half:], pairs)
        steps.append(held)
    x1, x2, x3 = x0 ^ 1, x0 ^ 2, x0 ^ 3
    for pairs in (
        [(at(0, core, k, x0), at(2, core, k, x0)) for k in cols],
        [(at(y, core, k, x0), at(y + 1, core, k, x0)) for k in cols for y in (0, 2)],
        [(at(y, core, k, x0), at(y, core, k, x2)) for k in cols for y in ys],
        [
            (at(y, core, k, a), at(y, core, k, b))
            for k in cols
            for y in ys
            for a, b in ((x0, x1), (x2, x3))
        ],
    ):
        held = wait(held)
        held = held + send(held, pairs)
        steps.append(held)
    for bit in (4, 2, 1):
        pairs = [(at(y, core, k, x), at(y, core, k ^ bit, x)) for k in cols for y in ys for x in xs]
        held = wait(held)
        held = jnp.concatenate([held, send(held, pairs)])
        steps.append(held)
    pairs = [(at(y, core, k, x), at(y, 1 - core, k, x)) for k in cols for y in ys for x in xs]
    held = wait(held)
    other = send(held, [p for p in pairs if p[1] not in skip])
    steps.append(other)
    return (held, other), steps


def body(matrix):
    mine = matrix[0, 0]
    size = mine.shape[0]
    r = lax.axis_index("row")
    z = lax.axis_index("col")
    c = lax.axis_index(("col", "depth"))
    me = lax.axis_index(AXES)
    owner = me == OWNER
    place = jnp.stack([c, r, owner.astype(jnp.int32), z]).astype(jnp.int32)
    flag = owner.astype(jnp.int32).reshape(1)

    inv0, packed0, up0, tick = factor(first_kernel, flag, mine)
    f10 = send(mine, [(ROOT, OWNER)])
    f11 = send(mine, [(dev(1, 1), OWNER)])

    step = size // 8
    after = later(mine, tick)
    got = []
    for k in range(8):
        pairs = [(dev(0, j), dev(j % 8, 8 * (j // 8) + k)) for j in range(1, N_BC)]
        pairs += [(dev(1, j), dev(j % 8, 8 * (j // 8) + (k + 4) % 8)) for j in range(1, N_BC)]
        got.append(send(after[k * step : (k + 1) * step], pairs))
    slot = c % 8
    first = sum(jnp.where(slot == k, got[k], 0.0) for k in range(8))
    second = sum(jnp.where(slot == (k + 4) % 8, got[k], 0.0) for k in range(8))
    shares, mine, f10, f11, packed0 = lax.optimization_barrier(
        (jnp.stack([first, second]), mine, f10, f11, packed0)
    )
    gathered = lax.all_gather(shares, ("col", "depth"))

    root0 = send(packed0, [(OWNER, ROOT)])
    _, packed1, _, tick = factor(second_kernel, flag, inv0, f10, f11)
    root1 = send(packed1, [(OWNER, ROOT)])
    cross, cross_steps = broadcast(later(mine, tick).reshape(8, step, size), me, 0, 1)
    first, steps = broadcast(root0, me, 1, 0, (OWNER,))
    spread = steps[6]
    second, _ = broadcast(root1, me, 1, 0, (OWNER,), steps, steps[5])

    cs = range(2, N_BC)
    line = later(jnp.where(r < 2, mine, 0.0), cross_steps[4])
    line = line + send(line, [(dev(a, j), dev(a + 2, j)) for j in cs for a in (0, 1)])
    line = later(line, spread)
    hops = [(0, 6), (1, 7), (2, 4), (3, 5)]
    line = line + send(line, [(dev(a, j), dev(b, j)) for j in cs for a, b in hops])
    swap = send(line, [(dev(a, j), dev(a ^ 1, j)) for j in cs for a in range(8)])

    block = (size, size)
    x0, link, rest = multipliers(
        middle_kernel, [block] * 3, jnp.float32, [block] * 2, place, line, swap, packed0, *first, *cross
    )
    high, low = multipliers(
        tail_kernel, [(2,) + block] * 2, jnp.bfloat16, [block], place, packed1, *second, x0, link, rest
    )
    return last(place, gathered, high, low, matrix, up0)


def solution(mesh):
    placed = P(None, "row", None, ("col", "depth"))
    return jax.shard_map(body, mesh=mesh, in_specs=(placed,), out_specs=placed, check_vma=False)
```
